32 devices in a mesh: rows: 16 (over z, y, x), sub: 2 (over core).
Axes of the slice: x: 2, y: 2, z: 4, core: 2. Of those that a mesh axis runs over, the one named last changes fastest.
Arguments:
- matrix: float32 [4096, 384], P(('rows', 'sub')), as said below
- grad_out: float32 [4096, 384], P(('rows', 'sub')), as said below
- grad_factor: float32 [384, 384], replicated, may hold values from -6 to 6
Outputs:
- grad_matrix: float32 [4096, 384], P(('rows', 'sub'))
The draws below stay inside these ranges and needn't reach their ends.
Inputs may be any that keep to these rules, and one draw needn't show every extreme that they name: `matrix`: entries at most of order 1 / sqrt(4096), with a scale that varies by row and by column. `grad_out`: entries of order 0.01.
All inputs are finite; a program needn't handle non-finite values.
Results may differ from the reference program's by a relative error of at most 0.0004.
Values sent between devices are 32-bit elements; how exact they have to be, the bound alone decides.
A program may use at most 64 MiB of HBM per device.

```python
import jax
import jax.numpy as jnp
from jax import lax

N = 384
SECTIONS = 2
R_DEV = 128
ROWS = 4096


def column_mix(key):
    gaussian = jax.random.normal(jax.random.fold_in(key, 15), (N, N), jnp.float32)
    rotation = jnp.linalg.qr(gaussian)[0]
    position = jnp.arange(N, dtype=jnp.float32) / (N - 1)
    column_decay = jnp.power(jnp.float32(10.0), -4.0 * jnp.cbrt(position))
    return column_decay[:, None] * rotation


def shared_rows(key):
    blocks = ROWS // R_DEV
    base_rows = jax.random.normal(jax.random.fold_in(key, 11), (ROWS, N), jnp.float32)
    block_scale = jnp.exp(jax.random.uniform(jax.random.fold_in(key, 13), (blocks, 1), jnp.float32, -0.7, 0.7))
    row_scale = jnp.exp(jax.random.uniform(jax.random.fold_in(key, 14), (ROWS, 1), jnp.float32, -0.5, 0.5))
    scaled = jnp.repeat(block_scale, R_DEV, axis=0) * row_scale
    mixed = jnp.dot(base_rows * scaled, column_mix(key), precision=lax.Precision.HIGHEST, preferred_element_type=jnp.float32)
    return mixed / jnp.sqrt(jnp.float32(ROWS))


def draw_matrix(key, part):
    return shared_rows(key)


def draw_grad_out(key, part):
    noise_rows = jax.random.normal(jax.random.fold_in(key, 21), (ROWS, N), jnp.float32)
    return 0.01 * (noise_rows + 0.03 * jnp.sqrt(jnp.float32(ROWS)) * shared_rows(key))


def normal_values(stream_key, dims, scale, most, held_as=jnp.bfloat16):
    entries = jax.random.normal(stream_key, dims, jnp.float32) * scale
    return jnp.minimum(jnp.maximum(entries, -most), most).astype(held_as)


def setup_inputs(seed: int = 0) -> dict:
    arg_keys = jax.random.split(jax.random.key(seed), 4)
    return {
        "matrix": draw_matrix(jax.random.fold_in(arg_keys[3], 71), 0),
        "grad_out": draw_grad_out(jax.random.fold_in(arg_keys[3], 71), 0),
        "grad_factor": normal_values(arg_keys[2], (N, N), 1.0, 6.0, jnp.float32),
    }


shift_frac = 0.02

def full_dot(left, right):
    return jnp.dot(left.astype(jnp.float32), right.astype(jnp.float32), precision=lax.Precision.HIGHEST, preferred_element_type=jnp.float32)

def inner_gram(left, right):
    return lax.dot_general(left.astype(jnp.float32), right.astype(jnp.float32), (((0,), (0,)), ((), ())), precision=lax.Precision.HIGHEST, preferred_element_type=jnp.float32)

def cholesky_adjoint(lower_fac, lower_inv, lower_grad):
    product = full_dot(lower_fac.T, lower_grad)
    phi_part = jnp.tril(product) - 0.5 * jnp.diag(jnp.diag(product))
    sandwich = full_dot(full_dot(lower_inv.T, phi_part), lower_inv)
    return 0.5 * (sandwich + sandwich.T)

def factor_grads(uppers, grad_factor):
    count = len(uppers)
    result = []
    for section_index in range(count):
        middle = grad_factor
        for later in range(section_index + 1, count):
            middle = full_dot(uppers[later].T, middle)
        for earlier in range(section_index - 1, -1, -1):
            middle = full_dot(middle, uppers[earlier].T)
        result.append(middle)
    return result

def reference(matrix, grad_out, grad_factor):
    width = matrix.shape[1]
    rate = shift_frac / width
    identity = jnp.eye(width, dtype=jnp.float32)
    current = matrix
    saved = []
    for section_index in range(SECTIONS):
        summed = inner_gram(current, current)
        shift_val = rate * jnp.trace(summed)
        lower_fac = jnp.linalg.cholesky(summed + shift_val * identity)
        lower_inv = lax.linalg.triangular_solve(lower_fac, identity, left_side=True, lower=True)
        following = full_dot(current, lower_inv.T)
        saved.append((current, following, lower_fac, lower_inv))
        current = following
    uppers = [item[2].T for item in saved]
    fac_grads = factor_grads(uppers, grad_factor)
    q_grad = grad_out
    for section_index in range(SECTIONS - 1, -1, -1):
        before, after, lower_fac, lower_inv = saved[section_index]
        crossed = inner_gram(after, q_grad)
        total_grad = fac_grads[section_index] - full_dot(crossed, lower_inv)
        gram_grad = cholesky_adjoint(lower_fac, lower_inv, jnp.tril(total_grad.T))
        gram_grad = gram_grad + rate * jnp.trace(gram_grad) * identity
        q_grad = full_dot(q_grad, lower_inv) + 2.0 * full_dot(before, gram_grad)
    return q_grad
```

```python
import functools

import jax
import jax.numpy as jnp
from jax import lax
from jax.experimental import pallas as pl
from jax.experimental.pallas import tpu as pltpu
from jax.sharding import PartitionSpec as P

LANES = 128
PANEL = 16
SUBLANES = 8
shift_frac = 0.02
VMEM_LIMIT = 56 * 1024 * 1024


def dot(left, right, dims=((1,), (0,))):
    return lax.dot_general(
        left, right, (dims, ((), ())), precision=lax.Precision.HIGHEST, preferred_element_type=jnp.float32
    )


def halves(value):
    high = value.astype(jnp.bfloat16)
    return high, (value - high.astype(jnp.float32)).astype(jnp.bfloat16)


def dot3(left, right, dims=((1,), (0,))):
    (left_high, left_low), (right_high, right_low) = halves(left), halves(right)

    def product(a, b):
        return lax.dot_general(a, b, (dims, ((), ())), preferred_element_type=jnp.float32)

    return product(left_high, right_high) + (product(left_high, right_low) + product(left_low, right_high))


def dot3_tn(left, right):
    return dot3(left, right, ((0,), (0,)))


def dot3_nt(left, right):
    return dot3(left, right, ((1,), (1,)))


def dot_tn(left, right):
    return dot(left, right, ((0,), (0,)))


def dot_nt(left, right):
    return dot(left, right, ((1,), (1,)))


def upper_pairs(count):
    return [(i, j) for i in range(count) for j in range(i, count)]


def block(index):
    return pl.ds(index * LANES, LANES)


def iotas(shape):
    return lax.broadcasted_iota(jnp.int32, shape, 0), lax.broadcasted_iota(jnp.int32, shape, 1)


def piece_rows(rows, devices):
    share = -(-rows // devices)
    return -(-share // 8) * 8


class Summer:
    def __init__(self, counts, rows):
        self.counts, self.used = counts, rows
        self.devices = counts[0] * counts[1]
        self.piece = piece_rows(rows, self.devices)
        self.owners = -(-rows // self.piece)
        self.rows = self.owners * self.piece

    def scratch(self):
        return [
            pltpu.VMEM((self.rows, LANES), jnp.float32),
            pltpu.VMEM((self.devices - 1, self.piece, LANES), jnp.float32),
            pltpu.VMEM((self.rows, LANES), jnp.float32),
            pltpu.SemaphoreType.DMA((4,)),
        ]

    def bind(self, me, part, inbox, total, sems):
        self.me, self.part, self.inbox, self.total, self.sems = me, part, inbox, total, sems
        return self

    def peer(self, offset):
        return lax.rem(self.me + offset, self.devices)

    def place(self, device):
        return (device // self.counts[1], lax.rem(device, self.counts[1]))

    def rows_of(self, device):
        return pl.ds(pl.multiple_of(device * self.piece, 8), self.piece)

    def is_owner(self, device, action):
        if self.owners == self.devices:
            action()
        else:
            pl.when(device < self.owners)(action)

    def greet(self):
        barrier = pltpu.get_barrier_semaphore()

        def signal(offset, carry):
            pl.semaphore_signal(
                barrier, inc=1, device_id=self.place(self.peer(offset)), device_id_type=pl.DeviceIdType.MESH
            )
            return carry

        lax.fori_loop(1, self.devices, signal, 0)

    def greeted(self):
        pl.semaphore_wait(pltpu.get_barrier_semaphore(), self.devices - 1)

    def outgoing(self, offset):
        peer = self.peer(offset)
        return pltpu.make_async_remote_copy(
            src_ref=self.part.at[self.rows_of(peer)],
            dst_ref=self.inbox.at[offset - 1],
            send_sem=self.sems.at[0],
            recv_sem=self.sems.at[1],
            device_id=self.place(peer),
            device_id_type=pl.DeviceIdType.MESH,
        )

    def spread(self, offset):
        mine = self.total.at[self.rows_of(self.me)]
        return pltpu.make_async_remote_copy(
            src_ref=mine,
            dst_ref=mine,
            send_sem=self.sems.at[2],
            recv_sem=self.sems.at[3],
            device_id=self.place(self.peer(offset)),
            device_id_type=pl.DeviceIdType.MESH,
        )

    def each_peer(self, action):
        def step(offset, carry):
            action(offset)
            return carry

        lax.fori_loop(1, self.devices, step, 0)

    def start(self):
        if self.rows > self.used:
            spare = self.rows - self.used
            self.part[pl.ds(self.used, spare), :] = jnp.zeros((spare, LANES), jnp.float32)
        self.each_peer(lambda offset: self.is_owner(self.peer(offset), lambda: self.outgoing(offset).start()))

    def reduce(self):
        def owned():
            pltpu.make_async_copy(self.inbox, self.inbox, self.sems.at[1]).wait()
            mine = self.rows_of(self.me)
            summed = self.part[mine, :]
            for slot in range(self.devices - 1):
                summed = summed + self.inbox[slot]
            self.total[mine, :] = summed
            self.each_peer(lambda offset: self.spread(offset).start())

        self.is_owner(self.me, owned)

    def wait_rows(self, rows):
        view = self.total.at[pl.ds(0, rows)]
        pltpu.make_async_copy(view, view, self.sems.at[3]).wait()

    def finish(self):
        if self.owners == self.devices:
            self.wait_rows(self.rows - self.piece)
        else:
            pl.when(self.me < self.owners)(lambda: self.wait_rows(self.rows - self.piece))
            pl.when(self.me >= self.owners)(lambda: self.wait_rows(self.rows))
        self.each_peer(lambda offset: self.is_owner(self.peer(offset), lambda: self.outgoing(offset).wait_send()))
        self.is_owner(self.me, lambda: self.each_peer(lambda offset: self.spread(offset).wait_send()))


def store_gram(part, source, pairs):
    for index, (i, j) in enumerate(pairs):
        part[block(index), :] = dot_tn(source[:, block(i)], source[:, block(j)])


def thirds(value):
    high = value.astype(jnp.bfloat16)
    rest = value - high.astype(jnp.float32)
    middle = rest.astype(jnp.bfloat16)
    return high, middle, (rest - middle.astype(jnp.float32)).astype(jnp.bfloat16)


def packed_tn(left, right):
    (a, b, c), (d, e, f) = thirds(left), thirds(right)
    tall = jnp.concatenate([a, a, b, a, c, b], axis=0)
    wide = jnp.concatenate([d, e, d, f, d, e], axis=0)
    return lax.dot_general(tall, wide, (((0,), (0,)), ((), ())), preferred_element_type=jnp.float32)


def eliminate(pieces, first):
    sub, lane = iotas((SUBLANES, LANES))
    cols = [
        [jnp.broadcast_to(piece[0][:, first + k : first + k + 1], (SUBLANES, LANES)) for piece in pieces]
        for k in range(PANEL)
    ]
    roots = []
    for k in range(PANEL):
        own, at = k // SUBLANES, k % SUBLANES
        root = lax.rsqrt(cols[k][own][at : at + 1, :])
        roots.append(root)
        factors = {}
        for i in range(own, len(pieces)):
            factor = cols[k][i] * root
            if i > own:
                factors[i] = factor
            elif at < SUBLANES - 1:
                factors[i] = jnp.where(sub > at, factor, 0.0)
        for later in range(k + 1, PANEL):
            value = cols[later][own][at : at + 1, :] * root
            for i, factor in factors.items():
                cols[later][i] = cols[later][i] - factor * value
        for tile in range(2):
            row = pieces[own][tile][at : at + 1, :] * root
            for i, factor in factors.items():
                pieces[i][tile] = pieces[i][tile] - factor * row
    for own in range(PANEL // SUBLANES):
        scale = jnp.broadcast_to(roots[own * SUBLANES], (SUBLANES, LANES))
        for at in range(1, SUBLANES):
            scale = jnp.where(sub == at, roots[own * SUBLANES + at], scale)
        kept = lane >= first + own * SUBLANES + sub
        pieces[own][0] = jnp.where(kept, pieces[own][0] * scale, 0.0)
        pieces[own][1] = pieces[own][1] * scale


def factor_block(work):
    step, count = 2 * PANEL, PANEL // SUBLANES
    for top in range(0, LANES, step):
        pieces = []
        for row in range(top, top + step, SUBLANES):
            pieces.append([work[row : row + SUBLANES, 0:LANES], work[row : row + SUBLANES, LANES : 2 * LANES]])
        eliminate(pieces, top)
        done, pieces = pieces[:count], pieces[count:]
        eliminate(pieces, top + PANEL)
        done = done + pieces
        left = jnp.concatenate([piece[0] for piece in done], axis=0)
        right = jnp.concatenate([piece[1] for piece in done], axis=0)
        both = jnp.concatenate([left, right], axis=1)
        work[top : top + step, :] = both
        below = top + step
        if below < LANES:
            work[below:, :] = work[below:, :] - packed_tn(left, both)[below:, :]


def factor_all(width, gram, work, upper, inverse, after_block=lambda b: None):
    pairs = upper_pairs(width)
    size = width * LANES
    rate = shift_frac / size
    row, lane = iotas((LANES, LANES))
    same = row == lane
    trace = jnp.float32(0.0)
    for index, (i, j) in enumerate(pairs):
        if i == j:
            trace = trace + jnp.sum(jnp.where(same, gram[block(index), :], 0.0))
    shift = rate * trace
    eye = jnp.where(same, 1.0, 0.0).astype(jnp.float32)
    zero = jnp.zeros((LANES, LANES), jnp.float32)
    for index, (i, j) in enumerate(pairs):
        piece = gram[block(index), :]
        upper[block(i), block(j)] = piece + shift * eye if i == j else piece
        if i != j:
            upper[block(j), block(i)] = zero
            inverse[block(i), block(j)] = zero
    for b in range(width):
        work[:, pl.ds(0, LANES)] = upper[block(b), block(b)]
        work[:, pl.ds(LANES, LANES)] = eye
        factor_block(work)
        upper[block(b), block(b)] = work[:, pl.ds(0, LANES)]
        inv = work[:, pl.ds(LANES, LANES)]
        inverse[block(b), block(b)] = inv
        for j in range(b + 1, width):
            upper[block(b), block(j)] = dot(inv, upper[block(b), block(j)])
        for i in range(b + 1, width):
            for j in range(i, width):
                upper[block(i), block(j)] = upper[block(i), block(j)] - dot_tn(
                    upper[block(b), block(i)], upper[block(b), block(j)]
                )
        for j in range(b):
            acc = zero
            for k in range(j, b):
                acc = acc + dot_tn(upper[block(k), block(b)], inverse[block(k), block(j)])
            inverse[block(b), block(j)] = -dot(inv, acc)
        after_block(b)


def gram_grad(upper, inverse, total_grad, rate):
    row, lane = iotas(total_grad.shape)
    lower_grad = jnp.where(row >= lane, total_grad.T, 0.0)
    product = dot3(upper, lower_grad)
    phi = jnp.where(row > lane, product, jnp.where(row == lane, 0.5 * product, 0.0))
    sandwich = dot3(dot3_tn(inverse, phi), inverse)
    result = 0.5 * (sandwich + sandwich.T)
    trace = jnp.sum(jnp.where(row == lane, result, 0.0))
    return result + jnp.where(row == lane, rate * trace, 0.0)


def whole_kernel(counts, width, matrix, q_grad, grad_factor, out, *scratch):
    gram_sum, later_sum, cross_sum = scratch[0:4], scratch[4:8], scratch[8:12]
    work, upper1, inverse1, upper2, inverse2, current, square, held = scratch[12:]
    me = lax.axis_index("rows") * counts[1] + lax.axis_index("sub")
    pairs = upper_pairs(width)
    used = len(pairs) * LANES
    rate = shift_frac / (width * LANES)
    first = Summer(counts, used).bind(me, *gram_sum)
    second = Summer(counts, used).bind(me, *later_sum)
    cross = Summer(counts, width * width * LANES).bind(me, *cross_sum)

    first.greet()
    store_gram(first.part, matrix, pairs)
    first.greeted()
    first.start()
    first.reduce()
    first.finish()
    factor_all(width, first.total, work, upper1, inverse1)
    current[...] = dot_nt(matrix[...], inverse1[...])

    store_gram(second.part, current, pairs)
    second.start()
    for i in range(width):
        for j in range(width):
            cross.part[block(i * width + j), :] = dot_tn(current[:, block(i)], q_grad[:, block(j)])
    held[...] = dot3_nt(grad_factor[...], upper1[...])
    second.reduce()
    second.finish()
    cross.start()

    def after_block(b):
        if b == width - 2:
            cross.reduce()

    factor_all(width, second.total, work, upper2, inverse2, after_block)
    factor1 = dot3_tn(upper2[...], grad_factor[...])
    moved = dot3(q_grad[...], inverse2[...])
    cross.finish()
    for i in range(width):
        for j in range(width):
            square[block(i), block(j)] = cross.total[block(i * width + j), :]
    turned = dot3(square[...], inverse2[...])
    total2 = held[...] - dot3(inverse2[...], turned)
    grad2 = gram_grad(upper2[...], inverse2[...], total2, rate)
    for index, (i, j) in enumerate(pairs):
        piece = second.total[block(index), :]
        square[block(i), block(j)] = piece
        if i != j:
            square[block(j), block(i)] = piece.T
    crossed1 = turned + 2.0 * dot3(square[...], grad2)
    total1 = factor1 - dot3(crossed1, inverse1[...])
    grad1 = gram_grad(upper1[...], inverse1[...], total1, rate)
    middle = moved + 2.0 * dot3(current[...], grad2)
    out[...] = dot3(middle, inverse1[...]) + 2.0 * dot3(matrix[...], grad1)


def per_device(counts, matrix, grad_out, grad_factor):
    rows, size = matrix.shape
    width = size // LANES
    used = len(upper_pairs(width)) * LANES
    vmem = pl.BlockSpec(memory_space=pltpu.VMEM)
    square = pltpu.VMEM((size, size), jnp.float32)
    tall = pltpu.VMEM((rows, size), jnp.float32)
    work = pltpu.VMEM((LANES, 2 * LANES), jnp.float32)
    sums = (
        Summer(counts, used).scratch() + Summer(counts, used).scratch() + Summer(counts, width * size).scratch()
    )
    return pl.pallas_call(
        functools.partial(whole_kernel, counts, width),
        out_shape=jax.ShapeDtypeStruct((rows, size), jnp.float32),
        in_specs=[vmem] * 3,
        out_specs=vmem,
        scratch_shapes=sums + [work] + [square] * 4 + [tall, square, square],
        compiler_params=pltpu.CompilerParams(
            vmem_limit_bytes=VMEM_LIMIT, collective_id=0, has_side_effects=True
        ),
    )(matrix, grad_out, grad_factor)


def solution(mesh):
    counts = (mesh.shape["rows"], mesh.shape["sub"])
    placed = (P(("rows", "sub"), None), P(("rows", "sub"), None), P())
    return jax.shard_map(
        functools.partial(per_device, counts),
        mesh=mesh,
        in_specs=placed,
        out_specs=P(("rows", "sub"), None),
        check_vma=False,
    )
```

```python
import functools

import jax
import jax.numpy as jnp
from jax import lax
from jax.experimental import pallas as pl
from jax.experimental.pallas import tpu as pltpu
from jax.sharding import PartitionSpec as P

LANES = 128
PANEL = 16
SUBLANES = 8
shift_frac = 0.02
VMEM_LIMIT = 56 * 1024 * 1024


NN, NT, TN = ((1,), (0,)), ((1,), (1,)), ((0,), (0,))


def halves(value):
    high = value.astype(jnp.bfloat16)
    return high, (value - high.astype(jnp.float32)).astype(jnp.bfloat16)


def thirds(value):
    high = value.astype(jnp.bfloat16)
    rest = value - high.astype(jnp.float32)
    middle = rest.astype(jnp.bfloat16)
    return high, middle, (rest - middle.astype(jnp.float32)).astype(jnp.bfloat16)


def joined(left, right, dims):
    (left_axis,), (right_axis,) = dims
    left, right = jnp.concatenate(left, axis=left_axis), jnp.concatenate(right, axis=right_axis)
    return lax.dot_general(left, right, (dims, ((), ())), preferred_element_type=jnp.float32)


def dot6(left, right, dims=NN):
    (a, b, c), (d, e, f) = thirds(left), thirds(right)
    return joined([a, a, b, a, c, b], [d, e, d, f, d, e], dims)


def dot3(left, right, dims=NN):
    (a, b), (d, e) = halves(left), halves(right)
    return joined([a, a, b], [d, e, d], dims)


def upper_pairs(count):
    return [(i, j) for i in range(count) for j in range(i, count)]


def block(index):
    return pl.ds(index * LANES, LANES)


def iotas(shape):
    return lax.broadcasted_iota(jnp.int32, shape, 0), lax.broadcasted_iota(jnp.int32, shape, 1)


def piece_rows(rows, devices):
    share = -(-rows // devices)
    return -(-share // 8) * 8


class Summer:
    def __init__(self, counts, rows):
        self.counts, self.used = counts, rows
        self.devices = counts[0] * counts[1]
        self.piece = piece_rows(rows, self.devices)
        self.owners = -(-rows // self.piece)
        self.rows = self.owners * self.piece

    def scratch(self):
        return [
            pltpu.VMEM((self.rows, LANES), jnp.float32),
            pltpu.VMEM((self.devices - 1, self.piece, LANES), jnp.float32),
            pltpu.VMEM((self.rows, LANES), jnp.float32),
            pltpu.SemaphoreType.DMA((4,)),
        ]

    def bind(self, me, part, inbox, total, sems):
        self.me, self.part, self.inbox, self.total, self.sems = me, part, inbox, total, sems
        return self

    def peer(self, offset):
        return lax.rem(self.me + offset, self.devices)

    def place(self, device):
        return (device // self.counts[1], lax.rem(device, self.counts[1]))

    def rows_of(self, device):
        return pl.ds(pl.multiple_of(device * self.piece, 8), self.piece)

    def is_owner(self, device, action):
        if self.owners == self.devices:
            action()
        else:
            pl.when(device < self.owners)(action)

    def greet(self):
        barrier = pltpu.get_barrier_semaphore()

        def signal(offset, carry):
            pl.semaphore_signal(
                barrier, inc=1, device_id=self.place(self.peer(offset)), device_id_type=pl.DeviceIdType.MESH
            )
            return carry

        lax.fori_loop(1, self.devices, signal, 0)

    def greeted(self):
        pl.semaphore_wait(pltpu.get_barrier_semaphore(), self.devices - 1)

    def outgoing(self, offset):
        peer = self.peer(offset)
        return pltpu.make_async_remote_copy(
            src_ref=self.part.at[self.rows_of(peer)],
            dst_ref=self.inbox.at[offset - 1],
            send_sem=self.sems.at[0],
            recv_sem=self.sems.at[1],
            device_id=self.place(peer),
            device_id_type=pl.DeviceIdType.MESH,
        )

    def spread(self, offset):
        mine = self.total.at[self.rows_of(self.me)]
        return pltpu.make_async_remote_copy(
            src_ref=mine,
            dst_ref=mine,
            send_sem=self.sems.at[2],
            recv_sem=self.sems.at[3],
            device_id=self.place(self.peer(offset)),
            device_id_type=pl.DeviceIdType.MESH,
        )

    def each_peer(self, action):
        def step(offset, carry):
            action(offset)
            return carry

        lax.fori_loop(1, self.devices, step, 0)

    def start(self):
        if self.rows > self.used:
            spare = self.rows - self.used
            self.part[pl.ds(self.used, spare), :] = jnp.zeros((spare, LANES), jnp.float32)
        self.each_peer(lambda offset: self.is_owner(self.peer(offset), lambda: self.outgoing(offset).start()))

    def reduce(self):
        def owned():
            pltpu.make_async_copy(self.inbox, self.inbox, self.sems.at[1]).wait()
            mine = self.rows_of(self.me)
            summed = self.part[mine, :]
            for slot in range(self.devices - 1):
                summed = summed + self.inbox[slot]
            self.total[mine, :] = summed
            self.each_peer(lambda offset: self.spread(offset).start())

        self.is_owner(self.me, owned)

    def wait_rows(self, rows):
        view = self.total.at[pl.ds(0, rows)]
        pltpu.make_async_copy(view, view, self.sems.at[3]).wait()

    def gathered(self):
        if self.owners == self.devices:
            self.wait_rows(self.rows - self.piece)
        else:
            pl.when(self.me < self.owners)(lambda: self.wait_rows(self.rows - self.piece))
            pl.when(self.me >= self.owners)(lambda: self.wait_rows(self.rows))

    def settle(self):
        self.each_peer(lambda offset: self.is_owner(self.peer(offset), lambda: self.outgoing(offset).wait_send()))
        self.is_owner(self.me, lambda: self.each_peer(lambda offset: self.spread(offset).wait_send()))


class Paired:
    def __init__(self, counts, rows):
        assert counts[1] == 2
        self.devices, self.used = counts[0], rows
        self.half = rows // 2
        self.piece = piece_rows(self.half, self.devices)
        self.owners = -(-self.half // self.piece)
        self.padded = self.owners * self.piece

    def scratch(self):
        return [
            pltpu.VMEM((2 * self.padded, LANES), jnp.float32),
            pltpu.VMEM((self.half, LANES), jnp.float32),
            pltpu.VMEM((self.devices - 1, self.piece, LANES), jnp.float32),
            pltpu.VMEM((2 * self.padded, LANES), jnp.float32),
            pltpu.SemaphoreType.DMA((8,)),
        ]

    def bind(self, row, core, part, box, inbox, total, sems):
        self.row, self.core, self.part, self.box, self.inbox, self.total, self.sems = (
            row, core, part, box, inbox, total, sems,
        )
        return self

    def spans(self, start, count):
        result, at = [], start
        while at < start + count:
            end = start + count if at >= self.half else min(self.half, start + count)
            place = at if at < self.half else self.padded + at - self.half
            result.append((place, at - start, end - at))
            at = end
        return result

    def put(self, index, value):
        for place, offset, rows in self.spans(index * LANES, LANES):
            self.part[pl.ds(place, rows), :] = value[offset : offset + rows, :]

    def get(self, index):
        pieces = [self.total[pl.ds(place, rows), :] for place, _, rows in self.spans(index * LANES, LANES)]
        return pieces[0] if len(pieces) == 1 else jnp.concatenate(pieces, axis=0)

    def half_of(self, core, rows):
        return pl.ds(pl.multiple_of(core * self.padded, 8), rows)

    def rows_of(self, device):
        return pl.ds(pl.multiple_of(self.core * self.padded + device * self.piece, 8), self.piece)

    def peer(self, offset):
        return lax.rem(self.row + offset, self.devices)

    def copy(self, source, target, sem, row, core):
        return pltpu.make_async_remote_copy(
            src_ref=source,
            dst_ref=target,
            send_sem=self.sems.at[sem],
            recv_sem=self.sems.at[sem + 1],
            device_id=(row, core),
            device_id_type=pl.DeviceIdType.MESH,
        )

    def pairing(self):
        return self.copy(self.part.at[self.half_of(1 - self.core, self.half)], self.box, 0, self.row, 1 - self.core)

    def outgoing(self, offset):
        return self.copy(
            self.part.at[self.rows_of(self.peer(offset))], self.inbox.at[offset - 1], 2, self.peer(offset), self.core
        )

    def spread(self, offset):
        mine = self.total.at[self.rows_of(self.row)]
        return self.copy(mine, mine, 4, self.peer(offset), self.core)

    def sharing(self):
        mine = self.total.at[self.half_of(self.core, self.padded)]
        return self.copy(mine, mine, 6, self.row, 1 - self.core)

    def each_peer(self, action):
        def step(offset, carry):
            action(offset)
            return carry

        lax.fori_loop(1, self.devices, step, 0)

    def is_owner(self, device, action):
        if self.owners == self.devices:
            action()
        else:
            pl.when(device < self.owners)(action)

    def pair_start(self):
        self.pairing().start()

    def pair_add(self):
        self.pairing().wait_recv()
        mine = self.half_of(self.core, self.half)
        self.part[mine, :] = self.part[mine, :] + self.box[...]
        if self.padded > self.half:
            spare = self.padded - self.half
            place = pl.ds(pl.multiple_of(self.core * self.padded + self.half, 8), spare)
            self.part[place, :] = jnp.zeros((spare, LANES), jnp.float32)

    def scatter(self):
        self.each_peer(lambda offset: self.is_owner(self.peer(offset), lambda: self.outgoing(offset).start()))

    def reduce(self):
        def owned():
            pltpu.make_async_copy(self.inbox, self.inbox, self.sems.at[3]).wait()
            mine = self.rows_of(self.row)
            summed = self.part[mine, :]
            for slot in range(self.devices - 1):
                summed = summed + self.inbox[slot]
            self.total[mine, :] = summed
            self.each_peer(lambda offset: self.spread(offset).start())

        self.is_owner(self.row, owned)

    def wait_rows(self, rows):
        view = self.total.at[pl.ds(0, rows)]
        pltpu.make_async_copy(view, view, self.sems.at[5]).wait()

    def share(self):
        if self.owners == self.devices:
            self.wait_rows(self.padded - self.piece)
        else:
            pl.when(self.row < self.owners)(lambda: self.wait_rows(self.padded - self.piece))
            pl.when(self.row >= self.owners)(lambda: self.wait_rows(self.padded))
        self.sharing().start()

    def shared(self):
        self.sharing().wait_recv()

    def settle(self):
        self.pairing().wait_send()
        self.each_peer(lambda offset: self.is_owner(self.peer(offset), lambda: self.outgoing(offset).wait_send()))
        self.is_owner(self.row, lambda: self.each_peer(lambda offset: self.spread(offset).wait_send()))
        self.sharing().wait_send()


def eliminate(pieces, first):
    sub, lane = iotas((SUBLANES, LANES))
    cols = [
        [jnp.broadcast_to(piece[0][:, first + k : first + k + 1], (SUBLANES, LANES)) for piece in pieces]
        for k in range(PANEL)
    ]
    roots = []
    for k in range(PANEL):
        own, at = k // SUBLANES, k % SUBLANES
        root = lax.rsqrt(cols[k][own][at : at + 1, :])
        roots.append(root)
        factors = {}
        for i in range(own, len(pieces)):
            factor = cols[k][i] * root
            if i > own:
                factors[i] = factor
            elif at < SUBLANES - 1:
                factors[i] = jnp.where(sub > at, factor, 0.0)
        for later in range(k + 1, PANEL):
            value = cols[later][own][at : at + 1, :] * root
            for i, factor in factors.items():
                cols[later][i] = cols[later][i] - factor * value
        for tile in range(2):
            row = pieces[own][tile][at : at + 1, :] * root
            for i, factor in factors.items():
                pieces[i][tile] = pieces[i][tile] - factor * row
    for own in range(PANEL // SUBLANES):
        scale = jnp.broadcast_to(roots[own * SUBLANES], (SUBLANES, LANES))
        for at in range(1, SUBLANES):
            scale = jnp.where(sub == at, roots[own * SUBLANES + at], scale)
        kept = lane >= first + own * SUBLANES + sub
        pieces[own][0] = jnp.where(kept, pieces[own][0] * scale, 0.0)
        pieces[own][1] = pieces[own][1] * scale


def factor_block(work):
    step, count = 2 * PANEL, PANEL // SUBLANES
    for top in range(0, LANES, step):
        pieces = []
        for row in range(top, top + step, SUBLANES):
            pieces.append([work[row : row + SUBLANES, 0:LANES], work[row : row + SUBLANES, LANES : 2 * LANES]])
        eliminate(pieces, top)
        done, pieces = pieces[:count], pieces[count:]
        eliminate(pieces, top + PANEL)
        done = done + pieces
        left = jnp.concatenate([piece[0] for piece in done], axis=0)
        right = jnp.concatenate([piece[1] for piece in done], axis=0)
        both = jnp.concatenate([left, right], axis=1)
        work[top : top + step, :] = both
        below = top + step
        if below < LANES:
            work[below:, :] = work[below:, :] - dot6(left, both, TN)[below:, :]


def upto(count):
    return pl.ds(0, count * LANES)


def factor_column(b, column, shift, work, upper, inverse):
    row, lane = iotas((LANES, LANES))
    eye = jnp.where(row == lane, 1.0, 0.0).astype(jnp.float32)
    diagonal = column[b] + shift * eye
    carried = None
    if b:
        above = jnp.concatenate(column[:b], axis=0)
        above = dot6(inverse[upto(b), upto(b)], above)
        upper[upto(b), block(b)] = above
        diagonal = diagonal - dot6(above, above, TN)
        carried = dot6(above, inverse[upto(b), upto(b)], TN)
    work[:, pl.ds(0, LANES)] = diagonal
    work[:, pl.ds(LANES, LANES)] = eye
    factor_block(work)
    upper[block(b), block(b)] = work[:, pl.ds(0, LANES)]
    inv = work[:, pl.ds(LANES, LANES)]
    inverse[block(b), block(b)] = inv
    zero = jnp.zeros((LANES, LANES), jnp.float32)
    for j in range(b):
        upper[block(b), block(j)] = zero
        inverse[block(j), block(b)] = zero
    if b:
        inverse[block(b), upto(b)] = -dot6(inv, carried)


def upper_times_lower(width, left, right, dot=dot3):
    columns = []
    for j in range(width):
        at = j * LANES
        columns.append(dot(left[0 : at + LANES, at:], right[at:, at : at + LANES]))
    return columns


def lower_times_upper(width, left, right, dot=dot3):
    rows = []
    for i in range(width):
        at = i * LANES
        rows.append(dot(left[at : at + LANES, 0 : at + LANES], right[0 : at + LANES, at:]))
    return rows


def from_columns(width, columns):
    size = width * LANES
    full = []
    for j, column in enumerate(columns):
        spare = size - column.shape[0]
        full.append(jnp.concatenate([column, jnp.zeros((spare, LANES), jnp.float32)], axis=0) if spare else column)
    return jnp.concatenate(full, axis=1)


def from_rows(width, rows):
    size = width * LANES
    full = []
    for row in rows:
        spare = size - row.shape[1]
        full.append(jnp.concatenate([jnp.zeros((LANES, spare), jnp.float32), row], axis=1) if spare else row)
    return jnp.concatenate(full, axis=0)


def symmetric_half(width, grad, upper):
    row, lane = iotas(grad.shape)
    kept = jnp.where(row <= lane, grad, 0.0)
    columns = []
    for j in range(width):
        at = j * LANES
        columns.append(dot3(kept[0 : at + LANES, at:], upper[at : at + LANES, at:], NT))
    product = from_columns(width, columns)
    phi = jnp.where(row < lane, product, jnp.where(row == lane, 0.5 * product, 0.0))
    return 0.5 * (phi + phi.T), phi


def whole_kernel(counts, width, matrix, q_grad, grad_factor, out, *scratch):
    scratch = list(scratch)

    def take(count):
        taken = scratch[:count]
        del scratch[:count]
        return taken

    row, core = lax.axis_index("rows"), lax.axis_index("sub")
    me = row * counts[1] + core
    size = width * LANES
    rate = shift_frac / size
    pairs = [(i, b) for b in range(width) for i in range(b + 1)]
    head, rest, later, cross = summers(counts, width)
    head.bind(me, *take(4))
    rest.bind(row, core, *take(5))
    for summer in later:
        summer.bind(me, *take(4))
    cross.bind(row, core, *take(5))
    work, upper1, inverse1, upper2, inverse2, current, held, early = scratch

    head.greet()
    head.part[block(0), :] = dot6(matrix[:, block(0)], matrix[:, block(0)], TN)
    squares = jnp.sum(matrix[...] * matrix[...])
    head.part[pl.ds(LANES, SUBLANES), :] = jnp.full((SUBLANES, LANES), squares, jnp.float32)
    for index, (i, j) in enumerate(pairs[1:]):
        rest.put(index, dot6(matrix[:, block(i)], matrix[:, block(j)], TN))
    for index, (i, j) in enumerate(pairs):
        cross.put(index, dot6(matrix[:, block(i)], q_grad[:, block(j)], TN))
    head.greeted()
    head.start()
    rest.pair_start()
    cross.pair_start()
    rest.pair_add()
    rest.scatter()
    cross.pair_add()
    head.reduce()
    rest.reduce()
    cross.scatter()
    head.gathered()
    shift1 = rate * head.total[pl.ds(LANES, SUBLANES), :][0:1, :]

    def section1(b):
        if b == 0:
            column = [head.total[block(0), :]]
        else:
            column = [rest.get(pairs.index((i, b)) - 1) for i in range(b + 1)]
        factor_column(b, column, shift1, work, upper1, inverse1)
        current[:, block(b)] = dot6(matrix[:, upto(b + 1)], inverse1[block(b), upto(b + 1)], NT)
        later[b].part[upto(b + 1), :] = dot6(current[:, upto(b + 1)], current[:, block(b)], TN)
        later[b].start()

    for b in range(width):
        section1(b)
        if b == 0:
            rest.share()
            cross.reduce()
            rest.shared()
        if b == 1:
            later[0].reduce()
            cross.share()
    inverse = inverse1[...]
    squares = jnp.sum(inverse * inverse)
    shift2 = rate * (size - shift1 * squares)
    for summer in later[1:-1]:
        summer.reduce()
    cross.shared()
    crossed = [[cross.get(pairs.index((i, j))) if i <= j else None for j in range(width)] for i in range(width)]
    crossed = from_rows(width, [jnp.concatenate(crossed[i][i:], axis=1) for i in range(width)])
    held[...] = from_rows(width, lower_times_upper(width, inverse1, crossed, dot6))
    early[...] = dot3(grad_factor[...], upper1[...], NT)
    for b in range(width):
        if b == 1 or width == 1:
            later[-1].reduce()
        later[b].gathered()
        column = [later[b].total[block(i), :] for i in range(b + 1)]
        factor_column(b, column, shift2, work, upper2, inverse2)

    row, lane = iotas((size, size))
    inverse = inverse2[...]
    turned = from_columns(width, upper_times_lower(width, held[...], inverse))
    total2 = early[...] - from_rows(width, lower_times_upper(width, inverse, turned))
    half2, _ = symmetric_half(width, total2, upper2)
    middle = dot3(half2, inverse)
    trace2 = rate * jnp.sum(middle * inverse)
    gram = from_columns(width, [summer.total[upto(b + 1), :] for b, summer in enumerate(later)])
    wide2 = jnp.concatenate([shift2] * width, axis=1)
    across = dot3(upper2[...] - wide2 * inverse, middle, TN)
    crossed1 = turned + 2.0 * (across + trace2 * gram)
    total1 = dot3(upper2[...], grad_factor[...], TN) - from_columns(
        width, upper_times_lower(width, crossed1, inverse1)
    )
    half1, phi1 = symmetric_half(width, total1, upper1)
    missing = jnp.where(row == lane, 1.0 - gram, -gram)
    trace1 = rate * jnp.sum(phi1 * missing) / shift1
    after = dot3(current[...], inverse, NT)
    grad = dot3(q_grad[...], inverse) + 2.0 * (dot3(after, middle) + trace2 * current[...])
    grad = grad + 2.0 * dot3(current[...], half1)
    wide1 = jnp.concatenate([trace1] * width, axis=1)
    out[...] = dot3(grad, inverse1[...]) + 2.0 * wide1 * matrix[...]
    for summer in [head, rest, *later, cross]:
        summer.settle()


def summers(counts, width):
    count = width * (width + 1) // 2
    later = [Summer(counts, (b + 1) * LANES) for b in range(width)]
    return Summer(counts, LANES + SUBLANES), Paired(counts, (count - 1) * LANES), later, Paired(counts, count * LANES)


def per_device(counts, matrix, grad_out, grad_factor):
    rows, size = matrix.shape
    width = size // LANES
    vmem = pl.BlockSpec(memory_space=pltpu.VMEM)
    square = pltpu.VMEM((size, size), jnp.float32)
    tall = pltpu.VMEM((rows, size), jnp.float32)
    work = pltpu.VMEM((LANES, 2 * LANES), jnp.float32)
    head, rest, later, cross = summers(counts, width)
    sums = []
    for summer in [head, rest, *later, cross]:
        sums = sums + summer.scratch()
    return pl.pallas_call(
        functools.partial(whole_kernel, counts, width),
        out_shape=jax.ShapeDtypeStruct((rows, size), jnp.float32),
        in_specs=[vmem] * 3,
        out_specs=vmem,
        scratch_shapes=sums + [work] + [square] * 4 + [tall, square, square],
        compiler_params=pltpu.CompilerParams(
            vmem_limit_bytes=VMEM_LIMIT, collective_id=0, has_side_effects=True
        ),
    )(matrix, grad_out, grad_factor)


def solution(mesh):
    counts = (mesh.shape["rows"], mesh.shape["sub"])
    placed = (P(("rows", "sub"), None), P(("rows", "sub"), None), P())
    return jax.shard_map(
        functools.partial(per_device, counts),
        mesh=mesh,
        in_specs=placed,
        out_specs=P(("rows", "sub"), None),
        check_vma=False,
    )
```

```python
import functools

import jax
import jax.numpy as jnp
from jax import lax
from jax.experimental import pallas as pl
from jax.experimental.pallas import tpu as pltpu
from jax.sharding import PartitionSpec as P

LANES = 128
PANEL = 16
GROUP = 5
SUBLANES = 8
shift_frac = 0.02
VMEM_LIMIT = 56 * 1024 * 1024


NN, NT, TN = ((1,), (0,)), ((1,), (1,)), ((0,), (0,))


def halves(value):
    high = value.astype(jnp.bfloat16)
    return high, (value - high.astype(jnp.float32)).astype(jnp.bfloat16)


def thirds(value):
    high = value.astype(jnp.bfloat16)
    rest = value - high.astype(jnp.float32)
    middle = rest.astype(jnp.bfloat16)
    return high, middle, (rest - middle.astype(jnp.float32)).astype(jnp.bfloat16)


def joined(left, right, dims):
    (left_axis,), (right_axis,) = dims
    left, right = jnp.concatenate(left, axis=left_axis), jnp.concatenate(right, axis=right_axis)
    return lax.dot_general(left, right, (dims, ((), ())), preferred_element_type=jnp.float32)


def dot6(left, right, dims=NN):
    (a, b, c), (d, e, f) = thirds(left), thirds(right)
    return joined([a, a, b, a, c, b], [d, e, d, f, d, e], dims)


def dot3(left, right, dims=NN):
    (a, b), (d, e) = halves(left), halves(right)
    return joined([a, a, b], [d, e, d], dims)


def upper_pairs(count):
    return [(i, j) for i in range(count) for j in range(i, count)]


def block(index):
    return pl.ds(index * LANES, LANES)


def iotas(shape):
    return lax.broadcasted_iota(jnp.int32, shape, 0), lax.broadcasted_iota(jnp.int32, shape, 1)


def piece_rows(rows, devices):
    share = -(-rows // devices)
    return -(-share // 8) * 8


def each_row(count, action):
    whole, left = divmod(count - 1, GROUP)

    def trip(index, carry):
        for k in range(GROUP):
            action(index * GROUP + (k + 1))
        return carry

    lax.fori_loop(0, whole, trip, 0)
    for k in range(left):
        action(whole * GROUP + k + 1)


def bytes_of(view, sem):
    pltpu.make_async_copy(view, view, sem).wait()


def greet(counts, row, core):
    barrier = pltpu.get_barrier_semaphore()

    def signal(target, place):
        pl.semaphore_signal(barrier, inc=1, device_id=(target, place), device_id_type=pl.DeviceIdType.MESH)

    def both(offset):
        peer = lax.rem(row + offset, counts[0])
        for place in range(counts[1]):
            signal(peer, place)

    each_row(counts[0], both)
    signal(row, 1 - core)


def greeted(counts):
    pl.semaphore_wait(pltpu.get_barrier_semaphore(), counts[0] * counts[1] - 1)


class Direct:
    def __init__(self, counts, rows):
        assert counts[1] == 2
        self.devices, self.used = counts[0], rows
        self.piece = piece_rows(rows, self.devices)
        self.owners = -(-rows // self.piece)

    def scratch(self):
        return [
            pltpu.VMEM((self.owners * self.piece, LANES), jnp.float32),
            pltpu.VMEM((2 * self.devices - 1, self.piece, LANES), jnp.float32),
            pltpu.VMEM((self.owners * self.piece, LANES), jnp.float32),
            pltpu.SemaphoreType.DMA((4,)),
        ]

    def bind(self, row, core, part, inbox, total, sems):
        self.row, self.core, self.part, self.inbox, self.total, self.sems = row, core, part, inbox, total, sems
        return self

    def put(self, value):
        self.part[pl.ds(0, self.used), :] = value
        spare = self.owners * self.piece - self.used
        if spare:
            self.part[pl.ds(self.used, spare), :] = jnp.zeros((spare, LANES), jnp.float32)

    def get(self, start, count):
        return self.total[pl.ds(start, count), :]

    def peer(self, offset):
        return lax.rem(self.row + offset, self.devices)

    def rows_of(self, device):
        return pl.ds(pl.multiple_of(device * self.piece, 8), self.piece)

    def is_owner(self, row, action):
        if self.owners == self.devices:
            action()
        else:
            pl.when(row < self.owners)(action)

    def copy(self, source, target, sem, row, core):
        return pltpu.make_async_remote_copy(
            src_ref=source,
            dst_ref=target,
            send_sem=self.sems.at[sem],
            recv_sem=self.sems.at[sem + 1],
            device_id=(row, core),
            device_id_type=pl.DeviceIdType.MESH,
        )

    def outgoing(self, row, slot):
        return self.copy(self.part.at[self.rows_of(row)], self.inbox.at[slot], 0, row, 1)

    def spread(self, row, core):
        mine = self.total.at[self.rows_of(self.row)]
        return self.copy(mine, mine, 2, row, core)

    def start(self):
        def send(offset):
            peer = self.peer(offset)
            self.is_owner(peer, lambda: self.outgoing(peer, 2 * offset + self.core - 1).start())

        pl.when(self.core == 0)(lambda: self.is_owner(self.row, lambda: self.outgoing(self.row, 0).start()))
        each_row(self.devices, send)

    def owned(self, action):
        pl.when(self.core == 1)(lambda: self.is_owner(self.row, action))

    def reduce(self):
        def summed():
            bytes_of(self.inbox, self.sems.at[1])
            mine = self.rows_of(self.row)
            terms = [self.part[mine, :]] + [self.inbox[slot] for slot in range(2 * self.devices - 1)]
            while len(terms) > 1:
                odd = terms[len(terms) // 2 * 2 :]
                terms = [terms[k] + terms[k + 1] for k in range(0, len(terms) - 1, 2)] + odd
            self.total[mine, :] = terms[0]

            def send(offset):
                for core in (1, 0):
                    self.spread(self.peer(offset), core).start()

            each_row(self.devices, send)
            self.spread(self.row, 0).start()

        self.owned(summed)

    def gathered(self):
        rows = self.owners * self.piece
        full = self.total.at[pl.ds(0, rows)]
        if self.owners == self.devices:
            pl.when(self.core == 0)(lambda: bytes_of(full, self.sems.at[3]))
            others = self.total.at[pl.ds(0, rows - self.piece)]
            pl.when(self.core == 1)(lambda: bytes_of(others, self.sems.at[3]))
            return
        mine = (self.core == 1) & (self.row < self.owners)
        if self.owners > 1:
            others = self.total.at[pl.ds(0, rows - self.piece)]
            pl.when(mine)(lambda: bytes_of(others, self.sems.at[3]))
        pl.when(jnp.logical_not(mine))(lambda: bytes_of(full, self.sems.at[3]))

    def settle(self):
        rows = self.owners * self.piece
        full = self.part.at[pl.ds(0, rows)]
        if self.owners == self.devices:
            pl.when(self.core == 0)(lambda: bytes_of(full, self.sems.at[0]))
            others = self.part.at[pl.ds(0, rows - self.piece)]
            pl.when(self.core == 1)(lambda: bytes_of(others, self.sems.at[0]))
        else:
            mine = self.row < self.owners
            keeps = (self.core == 1) & mine
            if self.owners > 1:
                others = self.part.at[pl.ds(0, rows - self.piece)]
                pl.when(keeps)(lambda: bytes_of(others, self.sems.at[0]))
            pl.when(jnp.logical_not(keeps))(lambda: bytes_of(full, self.sems.at[0]))
        self.owned(lambda: bytes_of(self.inbox, self.sems.at[2]))


class Paired:
    def __init__(self, counts, rows):
        assert counts[1] == 2
        self.devices, self.used = counts[0], rows
        self.half = rows // 2
        self.piece = piece_rows(self.half, self.devices)
        self.owners = -(-self.half // self.piece)
        self.padded = self.owners * self.piece

    def scratch(self):
        return [
            pltpu.VMEM((2 * self.padded, LANES), jnp.float32),
            pltpu.VMEM((self.half, LANES), jnp.float32),
            pltpu.VMEM((self.devices - 1, self.piece, LANES), jnp.float32),
            pltpu.VMEM((2 * self.padded, LANES), jnp.float32),
            pltpu.SemaphoreType.DMA((8,)),
        ]

    def bind(self, row, core, part, box, inbox, total, sems):
        self.row, self.core, self.part, self.box, self.inbox, self.total, self.sems = (
            row, core, part, box, inbox, total, sems,
        )
        return self

    def spans(self, start, count):
        result, at = [], start
        while at < start + count:
            end = start + count if at >= self.half else min(self.half, start + count)
            place = at if at < self.half else self.padded + at - self.half
            result.append((place, at - start, end - at))
            at = end
        return result

    def put(self, index, value):
        for place, offset, rows in self.spans(index * LANES, LANES):
            self.part[pl.ds(place, rows), :] = value[offset : offset + rows, :]

    def get(self, index):
        pieces = [self.total[pl.ds(place, rows), :] for place, _, rows in self.spans(index * LANES, LANES)]
        return pieces[0] if len(pieces) == 1 else jnp.concatenate(pieces, axis=0)

    def half_of(self, core, rows):
        return pl.ds(pl.multiple_of(core * self.padded, 8), rows)

    def rows_of(self, device):
        return pl.ds(pl.multiple_of(self.core * self.padded + device * self.piece, 8), self.piece)

    def peer(self, offset):
        return lax.rem(self.row + offset, self.devices)

    def copy(self, source, target, sem, row, core):
        return pltpu.make_async_remote_copy(
            src_ref=source,
            dst_ref=target,
            send_sem=self.sems.at[sem],
            recv_sem=self.sems.at[sem + 1],
            device_id=(row, core),
            device_id_type=pl.DeviceIdType.MESH,
        )

    def pairing(self):
        return self.copy(self.part.at[self.half_of(1 - self.core, self.half)], self.box, 0, self.row, 1 - self.core)

    def outgoing(self, offset):
        return self.copy(
            self.part.at[self.rows_of(self.peer(offset))], self.inbox.at[offset - 1], 2, self.peer(offset), self.core
        )

    def spread(self, offset):
        mine = self.total.at[self.rows_of(self.row)]
        return self.copy(mine, mine, 4, self.peer(offset), self.core)

    def sharing(self):
        mine = self.total.at[self.half_of(self.core, self.padded)]
        return self.copy(mine, mine, 6, self.row, 1 - self.core)

    def is_owner(self, device, action):
        if self.owners == self.devices:
            action()
        else:
            pl.when(device < self.owners)(action)

    def pair_start(self):
        self.pairing().start()

    def pair_add(self):
        self.pairing().wait_recv()
        mine = self.half_of(self.core, self.half)
        self.part[mine, :] = self.part[mine, :] + self.box[...]
        if self.padded > self.half:
            spare = self.padded - self.half
            place = pl.ds(pl.multiple_of(self.core * self.padded + self.half, 8), spare)
            self.part[place, :] = jnp.zeros((spare, LANES), jnp.float32)

    def scatter(self):
        each_row(self.devices, lambda offset: self.is_owner(self.peer(offset), lambda: self.outgoing(offset).start()))

    def reduce(self):
        def owned():
            bytes_of(self.inbox, self.sems.at[3])
            mine = self.rows_of(self.row)
            summed = self.part[mine, :]
            for slot in range(self.devices - 1):
                summed = summed + self.inbox[slot]
            self.total[mine, :] = summed
            each_row(self.devices, lambda offset: self.spread(offset).start())

        self.is_owner(self.row, owned)

    def wait_rows(self, rows):
        view = self.total.at[pl.ds(0, rows)]
        pltpu.make_async_copy(view, view, self.sems.at[5]).wait()

    def share(self):
        if self.owners == self.devices:
            self.wait_rows(self.padded - self.piece)
        else:
            pl.when(self.row < self.owners)(lambda: self.wait_rows(self.padded - self.piece))
            pl.when(self.row >= self.owners)(lambda: self.wait_rows(self.padded))
        self.sharing().start()

    def shared(self):
        self.sharing().wait_recv()

    def settle(self):
        self.pairing().wait_send()
        if self.owners == self.devices:
            bytes_of(self.inbox, self.sems.at[2])
        else:
            rows = self.padded - self.piece
            if rows:
                pl.when(self.row < self.owners)(lambda: bytes_of(self.part.at[pl.ds(0, rows)], self.sems.at[2]))
            full = self.part.at[pl.ds(0, self.padded)]
            pl.when(self.row >= self.owners)(lambda: bytes_of(full, self.sems.at[2]))
        self.is_owner(self.row, lambda: bytes_of(self.inbox, self.sems.at[4]))
        self.sharing().wait_send()


def eliminate(pieces, first):
    sub, lane = iotas((SUBLANES, LANES))
    cols = [
        [jnp.broadcast_to(piece[0][:, first + k : first + k + 1], (SUBLANES, LANES)) for piece in pieces]
        for k in range(PANEL)
    ]
    roots = []
    for k in range(PANEL):
        own, at = k // SUBLANES, k % SUBLANES
        root = lax.rsqrt(cols[k][own][at : at + 1, :])
        roots.append(root)
        factors = {}
        for i in range(own, len(pieces)):
            factor = cols[k][i] * root
            if i > own:
                factors[i] = factor
            elif at < SUBLANES - 1:
                factors[i] = jnp.where(sub > at, factor, 0.0)
        for later in range(k + 1, PANEL):
            value = cols[later][own][at : at + 1, :] * root
            for i, factor in factors.items():
                cols[later][i] = cols[later][i] - factor * value
        for tile in range(2):
            row = pieces[own][tile][at : at + 1, :] * root
            for i, factor in factors.items():
                pieces[i][tile] = pieces[i][tile] - factor * row
    for own in range(PANEL // SUBLANES):
        scale = jnp.broadcast_to(roots[own * SUBLANES], (SUBLANES, LANES))
        for at in range(1, SUBLANES):
            scale = jnp.where(sub == at, roots[own * SUBLANES + at], scale)
        kept = lane >= first + own * SUBLANES + sub
        pieces[own][0] = jnp.where(kept, pieces[own][0] * scale, 0.0)
        pieces[own][1] = pieces[own][1] * scale


def factor_block(work, hooks):
    step, count = 2 * PANEL, PANEL // SUBLANES
    for top in range(0, LANES, step):
        hooks.get(top // step, lambda: None)()
        pieces = []
        for row in range(top, top + step, SUBLANES):
            pieces.append([work[row : row + SUBLANES, 0:LANES], work[row : row + SUBLANES, LANES : 2 * LANES]])
        eliminate(pieces, top)
        done, pieces = pieces[:count], pieces[count:]
        eliminate(pieces, top + PANEL)
        done = done + pieces
        left = jnp.concatenate([piece[0] for piece in done], axis=0)
        right = jnp.concatenate([piece[1] for piece in done], axis=0)
        both = jnp.concatenate([left, right], axis=1)
        work[top : top + step, :] = both
        below = top + step
        if below < LANES:
            work[below:, :] = work[below:, :] - dot6(left, both, TN)[below:, :]


def upto(count):
    return pl.ds(0, count * LANES)


def prepare(b, above, upper, inverse):
    above = dot6(inverse[upto(b), upto(b)], above)
    upper[upto(b), block(b)] = above
    return dot6(above, above, TN), dot6(above, inverse[upto(b), upto(b)], TN)


def factor_column(b, diagonal, prepared, shift, work, upper, inverse, hooks):
    row, lane = iotas((LANES, LANES))
    eye = jnp.where(row == lane, 1.0, 0.0).astype(jnp.float32)
    diagonal = diagonal + shift * eye
    work[:, pl.ds(0, LANES)] = diagonal - prepared[0] if b else diagonal
    work[:, pl.ds(LANES, LANES)] = eye
    factor_block(work, hooks)
    upper[block(b), block(b)] = work[:, pl.ds(0, LANES)]
    inv = work[:, pl.ds(LANES, LANES)]
    inverse[block(b), block(b)] = inv
    zero = jnp.zeros((LANES, LANES), jnp.float32)
    for j in range(b):
        upper[block(b), block(j)] = zero
        inverse[block(j), block(b)] = zero
    if b:
        inverse[block(b), upto(b)] = -dot6(inv, prepared[1])


def upper_times_lower(width, left, right, dot=dot3):
    columns = []
    for j in range(width):
        at = j * LANES
        columns.append(dot(left[0 : at + LANES, at:], right[at:, at : at + LANES]))
    return columns


def lower_times_upper(width, left, right, dot=dot3):
    rows = []
    for i in range(width):
        at = i * LANES
        rows.append(dot(left[at : at + LANES, 0 : at + LANES], right[0 : at + LANES, at:]))
    return rows


def from_columns(width, columns):
    size = width * LANES
    full = []
    for j, column in enumerate(columns):
        spare = size - column.shape[0]
        full.append(jnp.concatenate([column, jnp.zeros((spare, LANES), jnp.float32)], axis=0) if spare else column)
    return jnp.concatenate(full, axis=1)


def from_rows(width, rows):
    size = width * LANES
    full = []
    for row in rows:
        spare = size - row.shape[1]
        full.append(jnp.concatenate([jnp.zeros((LANES, spare), jnp.float32), row], axis=1) if spare else row)
    return jnp.concatenate(full, axis=0)


def symmetric_half(width, grad, upper):
    row, lane = iotas(grad.shape)
    kept = jnp.where(row <= lane, grad, 0.0)
    columns = []
    for j in range(width):
        at = j * LANES
        columns.append(dot3(kept[0 : at + LANES, at:], upper[at : at + LANES, at:], NT))
    product = from_columns(width, columns)
    phi = jnp.where(row < lane, product, jnp.where(row == lane, 0.5 * product, 0.0))
    return 0.5 * (phi + phi.T), phi


def whole_kernel(counts, width, matrix_in, q_grad_in, grad_factor_in, out, *scratch):
    scratch = list(scratch)

    def take(count):
        taken = scratch[:count]
        del scratch[:count]
        return taken

    row, core = lax.axis_index("rows"), lax.axis_index("sub")
    size = width * LANES
    rate = shift_frac / size
    last = width - 1
    pairs = [(i, b) for b in range(width) for i in range(b + 1)]
    all_sums = summers(counts, width)
    head, rest, later, off, cross = all_sums
    for summer in flat(all_sums):
        summer.bind(row, core, *take(len(summer.scratch())))
    matrix, q_grad, grad_factor, loads, work, upper1, inverse1, upper2, inverse2, current, held, early = scratch

    loading = []
    for index, (source, target) in enumerate(
        [(matrix_in, matrix), (q_grad_in, q_grad), (grad_factor_in, grad_factor)]
    ):
        loading.append(pltpu.make_async_copy(source, target, loads.at[index]))
        loading[-1].start()
    greet(counts, row, core)
    loading[0].wait()
    squares = jnp.sum(matrix[...] * matrix[...])
    line, lane = iotas((LANES, LANES))
    corner = (line == LANES - 1) & (lane == 0)
    head.put(jnp.where(corner, squares, dot6(matrix[:, block(0)], matrix[:, block(0)], TN)))
    for b in range(1, width):
        for i in range(b + 1):
            rest[b - 1].put(i, dot6(matrix[:, block(i)], matrix[:, block(b)], TN))
    loading[1].wait()
    for index, (i, j) in enumerate(pairs):
        cross.put(index, dot6(matrix[:, block(i)], q_grad[:, block(j)], TN))
    loading[2].wait()
    greeted(counts)
    head.start()
    for summer in rest + [cross]:
        summer.pair_start()
    for summer in rest:
        summer.pair_add()
        summer.scatter()
    cross.pair_add()
    head.reduce()
    for summer in rest:
        summer.reduce()
    cross.scatter()
    head.gathered()
    first_block = head.get(0, LANES)
    shift1 = rate * jnp.broadcast_to(first_block[LANES - 1 : LANES, 0:1], (1, LANES))
    first_block = jnp.where(corner, first_block[0:1, LANES - 1 : LANES], first_block)

    def rest_share():
        for summer in rest[1:]:
            summer.share()

    def off_on():
        later[0].reduce()
        off.pair_add()
        off.scatter()

    hooks1 = {0: {2: lambda: rest[0].share()}, 1: {1: rest_share}, last: {1: off_on, 3: cross.share}}
    for b in range(width):
        if b == 0:
            diagonal, prepared = first_block, None
        else:
            rest[b - 1].shared()
            above = jnp.concatenate([rest[b - 1].get(i) for i in range(b)], axis=0)
            diagonal, prepared = rest[b - 1].get(b), prepare(b, above, upper1, inverse1)
        if b == last:
            ahead = matrix[:, block(b)] - dot6(matrix[:, upto(b)], prepared[1], NT)
            for i in range(b):
                off.put(i, dot6(current[:, block(i)], ahead, TN))
            off.pair_start()
        factor_column(b, diagonal, prepared, shift1, work, upper1, inverse1, hooks1.get(b, {}))
        current[:, block(b)] = dot6(matrix[:, upto(b + 1)], inverse1[block(b), upto(b + 1)], NT)
        first = b if b == last else 0
        later[b].put(dot6(current[:, first * LANES : (b + 1) * LANES], current[:, block(b)], TN))
        later[b].start()
        if b == 0:
            cross.reduce()
    for summer in later[1:-1]:
        summer.reduce()
    inverse = inverse1[...]
    shift2 = rate * (size - shift1 * jnp.sum(inverse * inverse))
    columns = []
    for j in range(width):
        at = j * LANES
        columns.append(dot3(grad_factor[0 : at + LANES, at:], upper1[at : at + LANES, at:], NT))
    early[...] = from_columns(width, columns)
    hooks2 = {0: {1: off.reduce}, 1: {2: off.share}}
    gram = []
    for b in range(width):
        if b == last:
            off.shared()
            above = jnp.concatenate([off.get(i) for i in range(b)], axis=0)
            above = dot6(above, inverse1[block(b), block(b)], NT)
            prepared = prepare(b, above, upper2, inverse2)
            later[b].gathered()
            diagonal = later[b].get(0, LANES)
            gram.append(jnp.concatenate([above, diagonal], axis=0))
        else:
            later[b].gathered()
            gram.append(later[b].get(0, (b + 1) * LANES))
            diagonal = gram[b][b * LANES :, :]
            prepared = prepare(b, gram[b][: b * LANES, :], upper2, inverse2) if b else None
        factor_column(b, diagonal, prepared, shift2, work, upper2, inverse2, hooks2.get(b, {}))
        if b == 0:
            later[-1].reduce()
            cross.shared()
            crossed = [
                jnp.concatenate([cross.get(pairs.index((i, j))) for j in range(i, width)], axis=1)
                for i in range(width)
            ]
            held[...] = from_rows(
                width, lower_times_upper(width, inverse1, from_rows(width, crossed), dot6)
            )

    row, lane = iotas((size, size))
    inverse = inverse2[...]
    turned = from_columns(width, upper_times_lower(width, held[...], inverse))
    total2 = early[...] - from_rows(width, lower_times_upper(width, inverse, turned))
    half2, _ = symmetric_half(width, total2, upper2)
    middle = jnp.concatenate(
        [dot3(half2[:, j * LANES :], inverse[j * LANES :, j * LANES : (j + 1) * LANES]) for j in range(width)], axis=1
    )
    trace2 = rate * jnp.sum(middle * inverse)
    gram = from_columns(width, gram)
    wide2 = jnp.concatenate([shift2] * width, axis=1)
    mixed = upper2[...] - wide2 * inverse
    across = from_columns(
        width,
        [
            dot3(mixed[:, 0 : (j + 1) * LANES], middle[:, j * LANES : (j + 1) * LANES], TN)
            for j in range(width)
        ],
    )
    crossed1 = turned + 2.0 * (across + trace2 * gram)
    moved = []
    for i in range(width):
        at = i * LANES
        moved.append(dot3(upper2[0 : at + LANES, at : at + LANES], grad_factor[0 : at + LANES, at:], TN))
    total1 = from_rows(width, moved) - from_columns(width, upper_times_lower(width, crossed1, inverse1))
    half1, phi1 = symmetric_half(width, total1, upper1)
    missing = jnp.where(row == lane, 1.0 - gram, -gram)
    trace1 = rate * jnp.sum(phi1 * missing) / shift1
    after = dot3(current[...], inverse, NT)
    grad = dot3(q_grad[...], inverse) + 2.0 * (dot3(after, middle) + trace2 * current[...])
    grad = grad + 2.0 * dot3(current[...], half1)
    wide1 = jnp.concatenate([trace1] * width, axis=1)
    out[...] = dot3(grad, inverse1[...]) + 2.0 * wide1 * matrix[...]
    for summer in flat(all_sums):
        summer.settle()


def summers(counts, width):
    count = width * (width + 1) // 2
    rest = [Paired(counts, (b + 1) * LANES) for b in range(1, width)]
    later = [Direct(counts, (b + 1) * LANES) for b in range(width - 1)] + [Direct(counts, LANES)]
    off = Paired(counts, (width - 1) * LANES)
    return Direct(counts, LANES), rest, later, off, Paired(counts, count * LANES)


def flat(sums):
    head, rest, later, off, cross = sums
    return [head, *rest, *later, off, cross]


def per_device(counts, matrix, grad_out, grad_factor):
    rows, size = matrix.shape
    width = size // LANES
    vmem = pl.BlockSpec(memory_space=pltpu.VMEM)
    square = pltpu.VMEM((size, size), jnp.float32)
    tall = pltpu.VMEM((rows, size), jnp.float32)
    work = pltpu.VMEM((LANES, 2 * LANES), jnp.float32)
    sums = []
    for summer in flat(summers(counts, width)):
        sums = sums + summer.scratch()
    held = [tall, tall, square, pltpu.SemaphoreType.DMA((3,)), work] + [square] * 4 + [tall, square, square]
    return pl.pallas_call(
        functools.partial(whole_kernel, counts, width),
        out_shape=jax.ShapeDtypeStruct((rows, size), jnp.float32),
        in_specs=[pl.BlockSpec(memory_space=pl.ANY)] * 3,
        out_specs=vmem,
        scratch_shapes=sums + held,
        compiler_params=pltpu.CompilerParams(
            vmem_limit_bytes=VMEM_LIMIT, collective_id=0, has_side_effects=True
        ),
    )(matrix, grad_out, grad_factor)


def solution(mesh):
    counts = (mesh.shape["rows"], mesh.shape["sub"])
    placed = (P(("rows", "sub"), None), P(("rows", "sub"), None), P())
    return jax.shard_map(
        functools.partial(per_device, counts),
        mesh=mesh,
        in_specs=placed,
        out_specs=P(("rows", "sub"), None),
        check_vma=False,
    )
```

```python
import functools

import jax
import jax.numpy as jnp
from jax import lax
from jax.experimental import pallas as pl
from jax.experimental.pallas import tpu as pltpu
from jax.sharding import PartitionSpec as P

LANES = 128
PANEL = 16
GROUP = 5
SUBLANES = 8
shift_frac = 0.02
VMEM_LIMIT = 56 * 1024 * 1024


NN, NT, TN = ((1,), (0,)), ((1,), (1,)), ((0,), (0,))


def halves(value):
    high = value.astype(jnp.bfloat16)
    return high, (value - high.astype(jnp.float32)).astype(jnp.bfloat16)


def thirds(value):
    high = value.astype(jnp.bfloat16)
    rest = value - high.astype(jnp.float32)
    middle = rest.astype(jnp.bfloat16)
    return high, middle, (rest - middle.astype(jnp.float32)).astype(jnp.bfloat16)


def joined(left, right, dims):
    (left_axis,), (right_axis,) = dims
    left, right = jnp.concatenate(left, axis=left_axis), jnp.concatenate(right, axis=right_axis)
    return lax.dot_general(left, right, (dims, ((), ())), preferred_element_type=jnp.float32)


def dot6(left, right, dims=NN):
    (a, b, c), (d, e, f) = thirds(left), thirds(right)
    return joined([a, a, b, a, c, b], [d, e, d, f, d, e], dims)


def dot3(left, right, dims=NN):
    (a, b), (d, e) = halves(left), halves(right)
    return joined([a, a, b], [d, e, d], dims)


def upper_pairs(count):
    return [(i, j) for i in range(count) for j in range(i, count)]


def block(index):
    return pl.ds(index * LANES, LANES)


def iotas(shape):
    return lax.broadcasted_iota(jnp.int32, shape, 0), lax.broadcasted_iota(jnp.int32, shape, 1)


def piece_rows(rows, devices):
    share = -(-rows // devices)
    return -(-share // 8) * 8


def each_row(count, action):
    whole, left = divmod(count - 1, GROUP)

    def trip(index, carry):
        for k in range(GROUP):
            action(index * GROUP + (k + 1))
        return carry

    lax.fori_loop(0, whole, trip, 0)
    for k in range(left):
        action(whole * GROUP + k + 1)


def bytes_of(view, sem):
    pltpu.make_async_copy(view, view, sem).wait()


def greet(counts, row, core):
    barrier = pltpu.get_barrier_semaphore()

    def signal(target, place):
        pl.semaphore_signal(barrier, inc=1, device_id=(target, place), device_id_type=pl.DeviceIdType.MESH)

    def both(offset):
        peer = lax.rem(row + offset, counts[0])
        for place in range(counts[1]):
            signal(peer, place)

    each_row(counts[0], both)
    signal(row, 1 - core)


def greeted(counts):
    pl.semaphore_wait(pltpu.get_barrier_semaphore(), counts[0] * counts[1] - 1)


class Direct:
    def __init__(self, counts, rows):
        assert counts[1] == 2
        self.devices, self.used = counts[0], rows
        self.piece = piece_rows(rows, self.devices)
        self.owners = -(-rows // self.piece)

    def scratch(self):
        return [
            pltpu.VMEM((self.owners * self.piece, LANES), jnp.float32),
            pltpu.VMEM((2 * self.devices - 1, self.piece, LANES), jnp.float32),
            pltpu.VMEM((self.owners * self.piece, LANES), jnp.float32),
            pltpu.SemaphoreType.DMA((4,)),
        ]

    def bind(self, row, core, part, inbox, total, sems):
        self.row, self.core, self.part, self.inbox, self.total, self.sems = row, core, part, inbox, total, sems
        return self

    def put(self, value):
        self.part[pl.ds(0, self.used), :] = value
        spare = self.owners * self.piece - self.used
        if spare:
            self.part[pl.ds(self.used, spare), :] = jnp.zeros((spare, LANES), jnp.float32)

    def get(self, start, count):
        return self.total[pl.ds(start, count), :]

    def peer(self, offset):
        return lax.rem(self.row + offset, self.devices)

    def rows_of(self, device):
        return pl.ds(pl.multiple_of(device * self.piece, 8), self.piece)

    def is_owner(self, row, action):
        if self.owners == self.devices:
            action()
        else:
            pl.when(row < self.owners)(action)

    def copy(self, source, target, sem, row, core):
        return pltpu.make_async_remote_copy(
            src_ref=source,
            dst_ref=target,
            send_sem=self.sems.at[sem],
            recv_sem=self.sems.at[sem + 1],
            device_id=(row, core),
            device_id_type=pl.DeviceIdType.MESH,
        )

    def outgoing(self, row, slot):
        return self.copy(self.part.at[self.rows_of(row)], self.inbox.at[slot], 0, row, 1)

    def spread(self, row, core):
        mine = self.total.at[self.rows_of(self.row)]
        return self.copy(mine, mine, 2, row, core)

    def start(self):
        def send(offset):
            peer = self.peer(offset)
            self.is_owner(peer, lambda: self.outgoing(peer, 2 * offset + self.core - 1).start())

        pl.when(self.core == 0)(lambda: self.is_owner(self.row, lambda: self.outgoing(self.row, 0).start()))
        each_row(self.devices, send)

    def owned(self, action):
        pl.when(self.core == 1)(lambda: self.is_owner(self.row, action))

    def reduce(self):
        def summed():
            bytes_of(self.inbox, self.sems.at[1])
            mine = self.rows_of(self.row)
            terms = [self.part[mine, :]] + [self.inbox[slot] for slot in range(2 * self.devices - 1)]
            while len(terms) > 1:
                odd = terms[len(terms) // 2 * 2 :]
                terms = [terms[k] + terms[k + 1] for k in range(0, len(terms) - 1, 2)] + odd
            self.total[mine, :] = terms[0]

            def send(offset):
                for core in (0, 1):
                    self.spread(self.peer(offset), core).start()

            each_row(self.devices, send)
            self.spread(self.row, 0).start()

        self.owned(summed)

    def gathered(self):
        rows = self.owners * self.piece
        full = self.total.at[pl.ds(0, rows)]
        if self.owners == self.devices:
            pl.when(self.core == 0)(lambda: bytes_of(full, self.sems.at[3]))
            others = self.total.at[pl.ds(0, rows - self.piece)]
            pl.when(self.core == 1)(lambda: bytes_of(others, self.sems.at[3]))
            return
        mine = (self.core == 1) & (self.row < self.owners)
        if self.owners > 1:
            others = self.total.at[pl.ds(0, rows - self.piece)]
            pl.when(mine)(lambda: bytes_of(others, self.sems.at[3]))
        pl.when(jnp.logical_not(mine))(lambda: bytes_of(full, self.sems.at[3]))

    def settle(self):
        rows = self.owners * self.piece
        full = self.part.at[pl.ds(0, rows)]
        if self.owners == self.devices:
            pl.when(self.core == 0)(lambda: bytes_of(full, self.sems.at[0]))
            others = self.part.at[pl.ds(0, rows - self.piece)]
            pl.when(self.core == 1)(lambda: bytes_of(others, self.sems.at[0]))
        else:
            mine = self.row < self.owners
            keeps = (self.core == 1) & mine
            if self.owners > 1:
                others = self.part.at[pl.ds(0, rows - self.piece)]
                pl.when(keeps)(lambda: bytes_of(others, self.sems.at[0]))
            pl.when(jnp.logical_not(keeps))(lambda: bytes_of(full, self.sems.at[0]))
        self.owned(lambda: bytes_of(self.inbox, self.sems.at[2]))


class Paired:
    def __init__(self, counts, rows):
        assert counts[1] == 2
        self.devices, self.used = counts[0], rows
        self.half = rows // 2
        self.piece = piece_rows(self.half, self.devices)
        self.owners = -(-self.half // self.piece)
        self.padded = self.owners * self.piece

    def scratch(self):
        return [
            pltpu.VMEM((2 * self.padded, LANES), jnp.float32),
            pltpu.VMEM((self.half, LANES), jnp.float32),
            pltpu.VMEM((self.devices - 1, self.piece, LANES), jnp.float32),
            pltpu.VMEM((2 * self.padded, LANES), jnp.float32),
            pltpu.SemaphoreType.DMA((8,)),
        ]

    def bind(self, row, core, part, box, inbox, total, sems):
        self.row, self.core, self.part, self.box, self.inbox, self.total, self.sems = (
            row, core, part, box, inbox, total, sems,
        )
        return self

    def spans(self, start, count):
        result, at = [], start
        while at < start + count:
            end = start + count if at >= self.half else min(self.half, start + count)
            place = at if at < self.half else self.padded + at - self.half
            result.append((place, at - start, end - at))
            at = end
        return result

    def put(self, index, value):
        for place, offset, rows in self.spans(index * LANES, LANES):
            self.part[pl.ds(place, rows), :] = value[offset : offset + rows, :]

    def get(self, index):
        pieces = [self.total[pl.ds(place, rows), :] for place, _, rows in self.spans(index * LANES, LANES)]
        return pieces[0] if len(pieces) == 1 else jnp.concatenate(pieces, axis=0)

    def half_of(self, core, rows):
        return pl.ds(pl.multiple_of(core * self.padded, 8), rows)

    def rows_of(self, device):
        return pl.ds(pl.multiple_of(self.core * self.padded + device * self.piece, 8), self.piece)

    def peer(self, offset):
        return lax.rem(self.row + offset, self.devices)

    def copy(self, source, target, sem, row, core):
        return pltpu.make_async_remote_copy(
            src_ref=source,
            dst_ref=target,
            send_sem=self.sems.at[sem],
            recv_sem=self.sems.at[sem + 1],
            device_id=(row, core),
            device_id_type=pl.DeviceIdType.MESH,
        )

    def pairing(self):
        return self.copy(self.part.at[self.half_of(1 - self.core, self.half)], self.box, 0, self.row, 1 - self.core)

    def outgoing(self, offset):
        return self.copy(
            self.part.at[self.rows_of(self.peer(offset))], self.inbox.at[offset - 1], 2, self.peer(offset), self.core
        )

    def spread(self, offset):
        mine = self.total.at[self.rows_of(self.row)]
        return self.copy(mine, mine, 4, self.peer(offset), self.core)

    def sharing(self):
        mine = self.total.at[self.half_of(self.core, self.padded)]
        return self.copy(mine, mine, 6, self.row, 1 - self.core)

    def is_owner(self, device, action):
        if self.owners == self.devices:
            action()
        else:
            pl.when(device < self.owners)(action)

    def pair_start(self):
        self.pairing().start()

    def pair_add(self):
        self.pairing().wait_recv()
        mine = self.half_of(self.core, self.half)
        self.part[mine, :] = self.part[mine, :] + self.box[...]
        if self.padded > self.half:
            spare = self.padded - self.half
            place = pl.ds(pl.multiple_of(self.core * self.padded + self.half, 8), spare)
            self.part[place, :] = jnp.zeros((spare, LANES), jnp.float32)

    def scatter(self):
        each_row(self.devices, lambda offset: self.is_owner(self.peer(offset), lambda: self.outgoing(offset).start()))

    def reduce(self):
        def owned():
            bytes_of(self.inbox, self.sems.at[3])
            mine = self.rows_of(self.row)
            summed = self.part[mine, :]
            for slot in range(self.devices - 1):
                summed = summed + self.inbox[slot]
            self.total[mine, :] = summed
            each_row(self.devices, lambda offset: self.spread(offset).start())

        self.is_owner(self.row, owned)

    def wait_rows(self, rows):
        view = self.total.at[pl.ds(0, rows)]
        pltpu.make_async_copy(view, view, self.sems.at[5]).wait()

    def share(self):
        if self.owners == self.devices:
            self.wait_rows(self.padded - self.piece)
        else:
            pl.when(self.row < self.owners)(lambda: self.wait_rows(self.padded - self.piece))
            pl.when(self.row >= self.owners)(lambda: self.wait_rows(self.padded))
        self.sharing().start()

    def shared(self):
        self.sharing().wait_recv()

    def settle(self):
        self.pairing().wait_send()
        if self.owners == self.devices:
            bytes_of(self.inbox, self.sems.at[2])
        else:
            rows = self.padded - self.piece
            if rows:
                pl.when(self.row < self.owners)(lambda: bytes_of(self.part.at[pl.ds(0, rows)], self.sems.at[2]))
            full = self.part.at[pl.ds(0, self.padded)]
            pl.when(self.row >= self.owners)(lambda: bytes_of(full, self.sems.at[2]))
        self.is_owner(self.row, lambda: bytes_of(self.inbox, self.sems.at[4]))
        self.sharing().wait_send()


def eliminate(pieces, first):
    sub, lane = iotas((SUBLANES, LANES))
    cols = [
        [jnp.broadcast_to(piece[0][:, first + k : first + k + 1], (SUBLANES, LANES)) for piece in pieces]
        for k in range(PANEL)
    ]
    roots = []
    for k in range(PANEL):
        own, at = k // SUBLANES, k % SUBLANES
        root = lax.rsqrt(cols[k][own][at : at + 1, :])
        roots.append(root)
        factors = {}
        for i in range(own, len(pieces)):
            factor = cols[k][i] * root
            if i > own:
                factors[i] = factor
            elif at < SUBLANES - 1:
                factors[i] = jnp.where(sub > at, factor, 0.0)
        for later in range(k + 1, PANEL):
            value = cols[later][own][at : at + 1, :] * root
            for i, factor in factors.items():
                cols[later][i] = cols[later][i] - factor * value
        for tile in range(2):
            row = pieces[own][tile][at : at + 1, :] * root
            for i, factor in factors.items():
                pieces[i][tile] = pieces[i][tile] - factor * row
    for own in range(PANEL // SUBLANES):
        scale = jnp.broadcast_to(roots[own * SUBLANES], (SUBLANES, LANES))
        for at in range(1, SUBLANES):
            scale = jnp.where(sub == at, roots[own * SUBLANES + at], scale)
        kept = lane >= first + own * SUBLANES + sub
        pieces[own][0] = jnp.where(kept, pieces[own][0] * scale, 0.0)
        pieces[own][1] = pieces[own][1] * scale


def factor_block(work, hooks):
    step, count = 2 * PANEL, PANEL // SUBLANES
    for top in range(0, LANES, step):
        hooks.get(top // step, lambda: None)()
        pieces = []
        for row in range(top, top + step, SUBLANES):
            pieces.append([work[row : row + SUBLANES, 0:LANES], work[row : row + SUBLANES, LANES : 2 * LANES]])
        eliminate(pieces, top)
        done, pieces = pieces[:count], pieces[count:]
        eliminate(pieces, top + PANEL)
        done = done + pieces
        left = jnp.concatenate([piece[0] for piece in done], axis=0)
        right = jnp.concatenate([piece[1] for piece in done], axis=0)
        both = jnp.concatenate([left, right], axis=1)
        work[top : top + step, :] = both
        below = top + step
        if below < LANES:
            work[below:, :] = work[below:, :] - dot6(left, both, TN)[below:, :]


def upto(count):
    return pl.ds(0, count * LANES)


def prepare(b, above, upper, inverse):
    above = dot6(inverse[upto(b), upto(b)], above)
    upper[upto(b), block(b)] = above
    return dot6(above, above, TN), dot6(above, inverse[upto(b), upto(b)], TN)


def factor_column(b, diagonal, prepared, shift, work, upper, inverse, hooks):
    row, lane = iotas((LANES, LANES))
    eye = jnp.where(row == lane, 1.0, 0.0).astype(jnp.float32)
    diagonal = diagonal + shift * eye
    work[:, pl.ds(0, LANES)] = diagonal - prepared[0] if b else diagonal
    work[:, pl.ds(LANES, LANES)] = eye
    factor_block(work, hooks)
    upper[block(b), block(b)] = work[:, pl.ds(0, LANES)]
    inv = work[:, pl.ds(LANES, LANES)]
    inverse[block(b), block(b)] = inv
    zero = jnp.zeros((LANES, LANES), jnp.float32)
    for j in range(b):
        upper[block(b), block(j)] = zero
        inverse[block(j), block(b)] = zero
    if b:
        inverse[block(b), upto(b)] = -dot6(inv, prepared[1])


def upper_times_lower(width, left, right, dot=dot3):
    columns = []
    for j in range(width):
        at = j * LANES
        columns.append(dot(left[0 : at + LANES, at:], right[at:, at : at + LANES]))
    return columns


def lower_times_upper(width, left, right, dot=dot3):
    rows = []
    for i in range(width):
        at = i * LANES
        rows.append(dot(left[at : at + LANES, 0 : at + LANES], right[0 : at + LANES, at:]))
    return rows


def from_columns(width, columns):
    size = width * LANES
    full = []
    for j, column in enumerate(columns):
        spare = size - column.shape[0]
        full.append(jnp.concatenate([column, jnp.zeros((spare, LANES), jnp.float32)], axis=0) if spare else column)
    return jnp.concatenate(full, axis=1)


def from_rows(width, rows):
    size = width * LANES
    full = []
    for row in rows:
        spare = size - row.shape[1]
        full.append(jnp.concatenate([jnp.zeros((LANES, spare), jnp.float32), row], axis=1) if spare else row)
    return jnp.concatenate(full, axis=0)


def symmetric_half(width, grad, upper):
    row, lane = iotas(grad.shape)
    kept = jnp.where(row <= lane, grad, 0.0)
    columns = []
    for j in range(width):
        at = j * LANES
        columns.append(dot3(kept[0 : at + LANES, at:], upper[at : at + LANES, at:], NT))
    product = from_columns(width, columns)
    phi = jnp.where(row < lane, product, jnp.where(row == lane, 0.5 * product, 0.0))
    return 0.5 * (phi + phi.T), phi


def whole_kernel(counts, width, matrix_in, q_grad_in, grad_factor_in, out, *scratch):
    scratch = list(scratch)

    def take(count):
        taken = scratch[:count]
        del scratch[:count]
        return taken

    row, core = lax.axis_index("rows"), lax.axis_index("sub")
    size = width * LANES
    rate = shift_frac / size
    last = width - 1
    pairs = [(i, b) for b in range(width) for i in range(b + 1)]
    all_sums = summers(counts, width)
    head, rest, later, off, cross = all_sums
    for summer in flat(all_sums):
        summer.bind(row, core, *take(len(summer.scratch())))
    matrix, q_grad, grad_factor, loads, work, upper1, inverse1, upper2, inverse2, current, held, early, gram2, moved, after, turning = scratch

    loading = []
    for index, (source, target) in enumerate(
        [(matrix_in, matrix), (q_grad_in, q_grad), (grad_factor_in, grad_factor)]
    ):
        loading.append(pltpu.make_async_copy(source, target, loads.at[index]))
        loading[-1].start()
    greet(counts, row, core)
    loading[0].wait()
    squares = jnp.sum(matrix[...] * matrix[...])
    line, lane = iotas((LANES, LANES))
    corner = (line == LANES - 1) & (lane == 0)
    head.put(jnp.where(corner, squares, dot6(matrix[:, block(0)], matrix[:, block(0)], TN)))
    greeted(counts)
    head.start()
    for b in range(1, width):
        for i in range(b + 1):
            rest[b - 1].put(i, dot6(matrix[:, block(i)], matrix[:, block(b)], TN))
        rest[b - 1].pair_start()
    loading[1].wait()
    for index, (i, j) in enumerate(pairs):
        cross.put(index, dot6(matrix[:, block(i)], q_grad[:, block(j)], TN))
    cross.pair_start()
    loading[2].wait()
    for summer in rest:
        summer.pair_add()
        summer.scatter()
    cross.pair_add()
    head.reduce()
    for summer in rest:
        summer.reduce()
    head.gathered()
    first_block = head.get(0, LANES)
    shift1 = rate * jnp.broadcast_to(first_block[LANES - 1 : LANES, 0:1], (1, LANES))
    first_block = jnp.where(corner, first_block[0:1, LANES - 1 : LANES], first_block)

    def rest_share():
        for summer in rest[1:]:
            summer.share()

    def between_on():
        for summer in later[1:-1]:
            summer.pair_add()
            summer.scatter()
        later[0].reduce()

    def off_on():
        off.pair_add()
        off.scatter()

    def gram1(b):
        above = jnp.concatenate([rest[b - 1].get(i) for i in range(b)], axis=0)
        return rest[b - 1].get(b), prepare(b, above, upper1, inverse1)

    hooks1 = {
        0: {2: rest[0].share},
        1: {1: rest_share},
        last: {0: between_on, 1: off_on},
    }
    diagonal, prepared = first_block, None
    for b in range(width):
        if b == last:
            ahead = matrix[:, block(b)] - dot6(matrix[:, upto(b)], prepared[1], NT)
            for i in range(b):
                off.put(i, dot6(current[:, block(i)], ahead, TN))
            off.pair_start()
        factor_column(b, diagonal, prepared, shift1, work, upper1, inverse1, hooks1.get(b, {}))
        if b < last:
            rest[b].shared()
        current[:, block(b)] = dot6(matrix[:, upto(b + 1)], inverse1[block(b), upto(b + 1)], NT)
        if b in (0, last):
            later[b].put(dot6(current[:, block(b)], current[:, block(b)], TN))
        else:
            for i in range(b + 1):
                later[b].put(i, dot6(current[:, block(i)], current[:, block(b)], TN))
        if b < last:
            diagonal, prepared = gram1(b + 1)
        if b in (0, last):
            later[b].start()
        else:
            later[b].pair_start()
        if b == 0:
            cross.scatter()
    for summer in later[1:-1]:
        summer.reduce()
    inverse = inverse1[...]
    shift2 = rate * (size - shift1 * jnp.sum(inverse * inverse))

    def early_on():
        columns = []
        for j in range(width):
            at = j * LANES
            columns.append(dot3(grad_factor[0 : at + LANES, at:], upper1[at : at + LANES, at:], NT))
        early[...] = from_columns(width, columns)

    def off_above():
        off.shared()
        above = jnp.concatenate([off.get(i) for i in range(last)], axis=0)
        gram2[upto(last), block(last)] = dot6(above, inverse1[block(last), block(last)], NT)

    def cross_on():
        cross.shared()
        crossed = [
            jnp.concatenate([cross.get(pairs.index((i, j))) for j in range(i, width)], axis=1) for i in range(width)
        ]
        held[...] = from_rows(width, lower_times_upper(width, inverse1, from_rows(width, crossed), dot6))

    def known_parts():
        for i in range(last):
            at = i * LANES
            moved[at : at + LANES, at:] = dot3(
                upper2[0 : at + LANES, at : at + LANES], grad_factor[0 : at + LANES, at:], TN
            )
        after[:, upto(last)] = dot3(current[:, upto(last)], inverse2[upto(last), upto(last)], NT)
        turning[:, upto(last)] = dot3(q_grad[:, upto(last)], inverse2[upto(last), upto(last)])

    hooks2 = {
        0: {1: early_on, 2: off.reduce, 3: cross.reduce},
        1: {2: off.share, 3: off_above},
        last: {1: cross.share, 2: known_parts, 3: cross_on},
    }
    for b in range(width):
        if b == last:
            prepared = prepare(b, gram2[upto(b), block(b)], upper2, inverse2)
            later[b].gathered()
            diagonal = later[b].get(0, LANES)
            gram2[block(b), block(b)] = diagonal
        else:
            if b:
                later[b].share()
                later[b].shared()
                column = jnp.concatenate([later[b].get(i) for i in range(b + 1)], axis=0)
            else:
                later[b].gathered()
                column = later[b].get(0, LANES)
            gram2[upto(b + 1), block(b)] = column
            diagonal = column[b * LANES :, :]
            prepared = prepare(b, column[: b * LANES, :], upper2, inverse2) if b else None
        factor_column(b, diagonal, prepared, shift2, work, upper2, inverse2, hooks2.get(b, {}))
        if b == 0:
            later[-1].reduce()

    row, lane = iotas((size, size))
    inverse = inverse2[...]
    turned = from_columns(width, upper_times_lower(width, held[...], inverse))
    total2 = early[...] - from_rows(width, lower_times_upper(width, inverse, turned))
    half2, _ = symmetric_half(width, total2, upper2)
    middle = jnp.concatenate(
        [dot3(half2[:, j * LANES :], inverse[j * LANES :, j * LANES : (j + 1) * LANES]) for j in range(width)], axis=1
    )
    trace2 = rate * jnp.sum(middle * inverse)
    gram = jnp.where(row // LANES <= lane // LANES, gram2[...], 0.0)
    wide2 = jnp.concatenate([shift2] * width, axis=1)
    mixed = upper2[...] - wide2 * inverse
    across = from_columns(
        width,
        [
            dot3(mixed[:, 0 : (j + 1) * LANES], middle[:, j * LANES : (j + 1) * LANES], TN)
            for j in range(width)
        ],
    )
    crossed1 = turned + 2.0 * (across + trace2 * gram)
    moved[block(last), block(last)] = dot3(upper2[:, block(last)], grad_factor[:, block(last)], TN)
    kept = jnp.where(row // LANES <= lane // LANES, moved[...], 0.0)
    total1 = kept - from_columns(width, upper_times_lower(width, crossed1, inverse1))
    half1, phi1 = symmetric_half(width, total1, upper1)
    missing = jnp.where(row == lane, 1.0 - gram, -gram)
    trace1 = rate * jnp.sum(phi1 * missing) / shift1
    after[:, block(last)] = dot3(current[...], inverse[last * LANES :, :], NT)
    turned_grad = dot3(q_grad[:, block(last)], inverse[last * LANES :, :])
    turned_grad = turned_grad + jnp.concatenate(
        [turning[:, upto(last)], jnp.zeros((q_grad.shape[0], LANES), jnp.float32)], axis=1
    )
    grad = turned_grad + 2.0 * (dot3(after[...], middle) + trace2 * current[...])
    grad = grad + 2.0 * dot3(current[...], half1)
    wide1 = jnp.concatenate([trace1] * width, axis=1)
    out[...] = dot3(grad, inverse1[...]) + 2.0 * wide1 * matrix[...]
    for summer in flat(all_sums):
        summer.settle()


def summers(counts, width):
    count = width * (width + 1) // 2
    rest = [Paired(counts, (b + 1) * LANES) for b in range(1, width)]
    later = [Direct(counts, LANES)] + [Paired(counts, (b + 1) * LANES) for b in range(1, width - 1)] + [Direct(counts, LANES)]
    off = Paired(counts, (width - 1) * LANES)
    return Direct(counts, LANES), rest, later, off, Paired(counts, count * LANES)


def flat(sums):
    head, rest, later, off, cross = sums
    return [head, *rest, *later, off, cross]


def per_device(counts, matrix, grad_out, grad_factor):
    rows, size = matrix.shape
    width = size // LANES
    vmem = pl.BlockSpec(memory_space=pltpu.VMEM)
    square = pltpu.VMEM((size, size), jnp.float32)
    tall = pltpu.VMEM((rows, size), jnp.float32)
    work = pltpu.VMEM((LANES, 2 * LANES), jnp.float32)
    sums = []
    for summer in flat(summers(counts, width)):
        sums = sums + summer.scratch()
    held = [tall, tall, square, pltpu.SemaphoreType.DMA((3,)), work] + [square] * 4 + [tall, square, square] + [square, square, tall, tall]
    return pl.pallas_call(
        functools.partial(whole_kernel, counts, width),
        out_shape=pltpu.VMEM((rows, size), jnp.float32),
        in_specs=[pl.BlockSpec(memory_space=pl.ANY)] * 3,
        out_specs=vmem,
        scratch_shapes=sums + held,
        compiler_params=pltpu.CompilerParams(
            vmem_limit_bytes=VMEM_LIMIT, collective_id=0, has_side_effects=True
        ),
    )(matrix, grad_out, grad_factor)


def solution(mesh):
    counts = (mesh.shape["rows"], mesh.shape["sub"])
    placed = (P(("rows", "sub"), None), P(("rows", "sub"), None), P())
    return jax.shard_map(
        functools.partial(per_device, counts),
        mesh=mesh,
        in_specs=placed,
        out_specs=P(("rows", "sub"), None),
        check_vma=False,
    )
```

```python
import functools

import jax
import jax.numpy as jnp
from jax import lax
from jax.experimental import pallas as pl
from jax.experimental.pallas import tpu as pltpu
from jax.sharding import PartitionSpec as P

LANES = 128
PANEL = 16
GROUP = 5
SUBLANES = 8
shift_frac = 0.02
VMEM_LIMIT = 56 * 1024 * 1024


NN, NT, TN = ((1,), (0,)), ((1,), (1,)), ((0,), (0,))


def halves(value):
    high = value.astype(jnp.bfloat16)
    return high, (value - high.astype(jnp.float32)).astype(jnp.bfloat16)


def thirds(value):
    high = value.astype(jnp.bfloat16)
    rest = value - high.astype(jnp.float32)
    middle = rest.astype(jnp.bfloat16)
    return high, middle, (rest - middle.astype(jnp.float32)).astype(jnp.bfloat16)


def joined(left, right, dims):
    (left_axis,), (right_axis,) = dims
    left, right = jnp.concatenate(left, axis=left_axis), jnp.concatenate(right, axis=right_axis)
    return lax.dot_general(left, right, (dims, ((), ())), preferred_element_type=jnp.float32)


def dot6(left, right, dims=NN):
    (a, b, c), (d, e, f) = thirds(left), thirds(right)
    return joined([a, a, b, a, c, b], [d, e, d, f, d, e], dims)


def dot3(left, right, dims=NN):
    (a, b), (d, e) = halves(left), halves(right)
    return joined([a, a, b], [d, e, d], dims)


def upper_pairs(count):
    return [(i, j) for i in range(count) for j in range(i, count)]


def block(index):
    return pl.ds(index * LANES, LANES)


def iotas(shape):
    return lax.broadcasted_iota(jnp.int32, shape, 0), lax.broadcasted_iota(jnp.int32, shape, 1)


def piece_rows(rows, devices):
    share = -(-rows // devices)
    return -(-share // 8) * 8


def each_row(count, action):
    whole, left = divmod(count - 1, GROUP)

    def trip(index, carry):
        for k in range(GROUP):
            action(index * GROUP + (k + 1))
        return carry

    lax.fori_loop(0, whole, trip, 0)
    for k in range(left):
        action(whole * GROUP + k + 1)


def bytes_of(view, sem):
    pltpu.make_async_copy(view, view, sem).wait()


def greet(counts, row, core):
    barrier = pltpu.get_barrier_semaphore()

    def signal(target, place):
        pl.semaphore_signal(barrier, inc=1, device_id=(target, place), device_id_type=pl.DeviceIdType.MESH)

    def both(offset):
        peer = lax.rem(row + offset, counts[0])
        for place in range(counts[1]):
            signal(peer, place)

    each_row(counts[0], both)
    signal(row, 1 - core)


def greeted(counts):
    pl.semaphore_wait(pltpu.get_barrier_semaphore(), counts[0] * counts[1] - 1)


class Direct:
    def __init__(self, counts, rows):
        assert counts[1] == 2
        self.devices, self.used = counts[0], rows
        self.piece = piece_rows(rows, self.devices)
        self.owners = -(-rows // self.piece)

    def scratch(self):
        return [
            pltpu.VMEM((self.owners * self.piece, LANES), jnp.float32),
            pltpu.VMEM((2 * self.devices - 1, self.piece, LANES), jnp.float32),
            pltpu.VMEM((self.owners * self.piece, LANES), jnp.float32),
            pltpu.SemaphoreType.DMA((4,)),
        ]

    def bind(self, row, core, part, inbox, total, sems):
        self.row, self.core, self.part, self.inbox, self.total, self.sems = row, core, part, inbox, total, sems
        return self

    def put(self, value):
        self.part[pl.ds(0, self.used), :] = value
        spare = self.owners * self.piece - self.used
        if spare:
            self.part[pl.ds(self.used, spare), :] = jnp.zeros((spare, LANES), jnp.float32)

    def get(self, start, count):
        return self.total[pl.ds(start, count), :]

    def peer(self, offset):
        return lax.rem(self.row + offset, self.devices)

    def rows_of(self, device):
        return pl.ds(pl.multiple_of(device * self.piece, 8), self.piece)

    def is_owner(self, row, action):
        if self.owners == self.devices:
            action()
        else:
            pl.when(row < self.owners)(action)

    def copy(self, source, target, sem, row, core):
        return pltpu.make_async_remote_copy(
            src_ref=source,
            dst_ref=target,
            send_sem=self.sems.at[sem],
            recv_sem=self.sems.at[sem + 1],
            device_id=(row, core),
            device_id_type=pl.DeviceIdType.MESH,
        )

    def outgoing(self, row, slot):
        return self.copy(self.part.at[self.rows_of(row)], self.inbox.at[slot], 0, row, 1)

    def spread(self, row, core):
        mine = self.total.at[self.rows_of(self.row)]
        return self.copy(mine, mine, 2, row, core)

    def start(self):
        def send(offset):
            peer = self.peer(offset)
            self.is_owner(peer, lambda: self.outgoing(peer, 2 * offset + self.core - 1).start())

        pl.when(self.core == 0)(lambda: self.is_owner(self.row, lambda: self.outgoing(self.row, 0).start()))
        each_row(self.devices, send)

    def owned(self, action):
        pl.when(self.core == 1)(lambda: self.is_owner(self.row, action))

    def reduce(self):
        def summed():
            bytes_of(self.inbox, self.sems.at[1])
            mine = self.rows_of(self.row)
            terms = [self.part[mine, :]] + [self.inbox[slot] for slot in range(2 * self.devices - 1)]
            while len(terms) > 1:
                odd = terms[len(terms) // 2 * 2 :]
                terms = [terms[k] + terms[k + 1] for k in range(0, len(terms) - 1, 2)] + odd
            self.total[mine, :] = terms[0]

            def send(offset):
                for core in (0, 1):
                    self.spread(self.peer(offset), core).start()

            each_row(self.devices, send)
            self.spread(self.row, 0).start()

        self.owned(summed)

    def gathered(self):
        rows = self.owners * self.piece
        full = self.total.at[pl.ds(0, rows)]
        if self.owners == self.devices:
            pl.when(self.core == 0)(lambda: bytes_of(full, self.sems.at[3]))
            others = self.total.at[pl.ds(0, rows - self.piece)]
            pl.when(self.core == 1)(lambda: bytes_of(others, self.sems.at[3]))
            return
        mine = (self.core == 1) & (self.row < self.owners)
        if self.owners > 1:
            others = self.total.at[pl.ds(0, rows - self.piece)]
            pl.when(mine)(lambda: bytes_of(others, self.sems.at[3]))
        pl.when(jnp.logical_not(mine))(lambda: bytes_of(full, self.sems.at[3]))

    def settle(self):
        rows = self.owners * self.piece
        full = self.part.at[pl.ds(0, rows)]
        if self.owners == self.devices:
            pl.when(self.core == 0)(lambda: bytes_of(full, self.sems.at[0]))
            others = self.part.at[pl.ds(0, rows - self.piece)]
            pl.when(self.core == 1)(lambda: bytes_of(others, self.sems.at[0]))
        else:
            mine = self.row < self.owners
            keeps = (self.core == 1) & mine
            if self.owners > 1:
                others = self.part.at[pl.ds(0, rows - self.piece)]
                pl.when(keeps)(lambda: bytes_of(others, self.sems.at[0]))
            pl.when(jnp.logical_not(keeps))(lambda: bytes_of(full, self.sems.at[0]))
        self.owned(lambda: bytes_of(self.inbox, self.sems.at[2]))


class Paired:
    def __init__(self, counts, rows):
        assert counts[1] == 2
        self.devices, self.used = counts[0], rows
        self.half = rows // 2
        self.piece = piece_rows(self.half, self.devices)
        self.owners = -(-self.half // self.piece)
        self.padded = self.owners * self.piece

    def scratch(self):
        return [
            pltpu.VMEM((2 * self.padded, LANES), jnp.float32),
            pltpu.VMEM((self.half, LANES), jnp.float32),
            pltpu.VMEM((self.devices - 1, self.piece, LANES), jnp.float32),
            pltpu.VMEM((2 * self.padded, LANES), jnp.float32),
            pltpu.SemaphoreType.DMA((8,)),
        ]

    def bind(self, row, core, part, box, inbox, total, sems):
        self.row, self.core, self.part, self.box, self.inbox, self.total, self.sems = (
            row, core, part, box, inbox, total, sems,
        )
        return self

    def spans(self, start, count):
        result, at = [], start
        while at < start + count:
            end = start + count if at >= self.half else min(self.half, start + count)
            place = at if at < self.half else self.padded + at - self.half
            result.append((place, at - start, end - at))
            at = end
        return result

    def put(self, index, value):
        for place, offset, rows in self.spans(index * LANES, LANES):
            self.part[pl.ds(place, rows), :] = value[offset : offset + rows, :]

    def get(self, index):
        pieces = [self.total[pl.ds(place, rows), :] for place, _, rows in self.spans(index * LANES, LANES)]
        return pieces[0] if len(pieces) == 1 else jnp.concatenate(pieces, axis=0)

    def half_of(self, core, rows):
        return pl.ds(pl.multiple_of(core * self.padded, 8), rows)

    def rows_of(self, device):
        return pl.ds(pl.multiple_of(self.core * self.padded + device * self.piece, 8), self.piece)

    def peer(self, offset):
        return lax.rem(self.row + offset, self.devices)

    def copy(self, source, target, sem, row, core):
        return pltpu.make_async_remote_copy(
            src_ref=source,
            dst_ref=target,
            send_sem=self.sems.at[sem],
            recv_sem=self.sems.at[sem + 1],
            device_id=(row, core),
            device_id_type=pl.DeviceIdType.MESH,
        )

    def pairing(self):
        return self.copy(self.part.at[self.half_of(1 - self.core, self.half)], self.box, 0, self.row, 1 - self.core)

    def outgoing(self, offset):
        return self.copy(
            self.part.at[self.rows_of(self.peer(offset))], self.inbox.at[offset - 1], 2, self.peer(offset), self.core
        )

    def spread(self, offset):
        mine = self.total.at[self.rows_of(self.row)]
        return self.copy(mine, mine, 4, self.peer(offset), self.core)

    def sharing(self):
        mine = self.total.at[self.half_of(self.core, self.padded)]
        return self.copy(mine, mine, 6, self.row, 1 - self.core)

    def is_owner(self, device, action):
        if self.owners == self.devices:
            action()
        else:
            pl.when(device < self.owners)(action)

    def pair_start(self):
        self.pairing().start()

    def pair_add(self):
        self.pairing().wait_recv()
        mine = self.half_of(self.core, self.half)
        self.part[mine, :] = self.part[mine, :] + self.box[...]
        if self.padded > self.half:
            spare = self.padded - self.half
            place = pl.ds(pl.multiple_of(self.core * self.padded + self.half, 8), spare)
            self.part[place, :] = jnp.zeros((spare, LANES), jnp.float32)

    def scatter(self):
        each_row(self.devices, lambda offset: self.is_owner(self.peer(offset), lambda: self.outgoing(offset).start()))

    def reduce(self):
        def owned():
            bytes_of(self.inbox, self.sems.at[3])
            mine = self.rows_of(self.row)
            summed = self.part[mine, :]
            for slot in range(self.devices - 1):
                summed = summed + self.inbox[slot]
            self.total[mine, :] = summed
            each_row(self.devices, lambda offset: self.spread(offset).start())

        self.is_owner(self.row, owned)

    def wait_rows(self, rows):
        view = self.total.at[pl.ds(0, rows)]
        pltpu.make_async_copy(view, view, self.sems.at[5]).wait()

    def share(self):
        if self.owners == self.devices:
            self.wait_rows(self.padded - self.piece)
        else:
            pl.when(self.row < self.owners)(lambda: self.wait_rows(self.padded - self.piece))
            pl.when(self.row >= self.owners)(lambda: self.wait_rows(self.padded))
        self.sharing().start()

    def shared(self):
        self.sharing().wait_recv()

    def settle(self):
        self.pairing().wait_send()
        if self.owners == self.devices:
            bytes_of(self.inbox, self.sems.at[2])
        else:
            rows = self.padded - self.piece
            if rows:
                pl.when(self.row < self.owners)(lambda: bytes_of(self.part.at[pl.ds(0, rows)], self.sems.at[2]))
            full = self.part.at[pl.ds(0, self.padded)]
            pl.when(self.row >= self.owners)(lambda: bytes_of(full, self.sems.at[2]))
        self.is_owner(self.row, lambda: bytes_of(self.inbox, self.sems.at[4]))
        self.sharing().wait_send()


def eliminate(pieces, first):
    sub, lane = iotas((SUBLANES, LANES))
    cols = [
        [jnp.broadcast_to(piece[0][:, first + k : first + k + 1], (SUBLANES, LANES)) for piece in pieces]
        for k in range(PANEL)
    ]
    roots = []
    for k in range(PANEL):
        own, at = k // SUBLANES, k % SUBLANES
        root = lax.rsqrt(cols[k][own][at : at + 1, :])
        roots.append(root)
        factors = {}
        for i in range(own, len(pieces)):
            factor = cols[k][i] * root
            if i > own:
                factors[i] = factor
            elif at < SUBLANES - 1:
                factors[i] = jnp.where(sub > at, factor, 0.0)
        for later in range(k + 1, PANEL):
            value = cols[later][own][at : at + 1, :] * root
            for i, factor in factors.items():
                cols[later][i] = cols[later][i] - factor * value
        for tile in range(2):
            row = pieces[own][tile][at : at + 1, :] * root
            for i, factor in factors.items():
                pieces[i][tile] = pieces[i][tile] - factor * row
    for own in range(PANEL // SUBLANES):
        scale = jnp.broadcast_to(roots[own * SUBLANES], (SUBLANES, LANES))
        for at in range(1, SUBLANES):
            scale = jnp.where(sub == at, roots[own * SUBLANES + at], scale)
        kept = lane >= first + own * SUBLANES + sub
        pieces[own][0] = jnp.where(kept, pieces[own][0] * scale, 0.0)
        pieces[own][1] = pieces[own][1] * scale


def factor_block(work, hooks):
    step, count = 2 * PANEL, PANEL // SUBLANES
    for top in range(0, LANES, step):
        hooks.get(top // step, lambda: None)()
        pieces = []
        for row in range(top, top + step, SUBLANES):
            pieces.append([work[row : row + SUBLANES, 0:LANES], work[row : row + SUBLANES, LANES : 2 * LANES]])
        eliminate(pieces, top)
        done, pieces = pieces[:count], pieces[count:]
        eliminate(pieces, top + PANEL)
        done = done + pieces
        left = jnp.concatenate([piece[0] for piece in done], axis=0)
        right = jnp.concatenate([piece[1] for piece in done], axis=0)
        both = jnp.concatenate([left, right], axis=1)
        work[top : top + step, :] = both
        below = top + step
        if below < LANES:
            work[below:, :] = work[below:, :] - dot6(left, both, TN)[below:, :]


def upto(count):
    return pl.ds(0, count * LANES)


def prepare(b, above, upper, inverse):
    above = dot6(inverse[upto(b), upto(b)], above)
    upper[upto(b), block(b)] = above
    return dot6(above, above, TN), dot6(above, inverse[upto(b), upto(b)], TN)


def factor_column(b, diagonal, prepared, shift, work, upper, inverse, hooks):
    row, lane = iotas((LANES, LANES))
    eye = jnp.where(row == lane, 1.0, 0.0).astype(jnp.float32)
    diagonal = diagonal + shift * eye
    work[:, pl.ds(0, LANES)] = diagonal - prepared[0] if b else diagonal
    work[:, pl.ds(LANES, LANES)] = eye
    factor_block(work, hooks)
    upper[block(b), block(b)] = work[:, pl.ds(0, LANES)]
    inv = work[:, pl.ds(LANES, LANES)]
    inverse[block(b), block(b)] = inv
    zero = jnp.zeros((LANES, LANES), jnp.float32)
    for j in range(b):
        upper[block(b), block(j)] = zero
        inverse[block(j), block(b)] = zero
    if b:
        inverse[block(b), upto(b)] = -dot6(inv, prepared[1])


def upper_times_lower(width, left, right, dot=dot3):
    columns = []
    for j in range(width):
        at = j * LANES
        columns.append(dot(left[0 : at + LANES, at:], right[at:, at : at + LANES]))
    return columns


def lower_times_upper(width, left, right, dot=dot3):
    rows = []
    for i in range(width):
        at = i * LANES
        rows.append(dot(left[at : at + LANES, 0 : at + LANES], right[0 : at + LANES, at:]))
    return rows


def from_columns(width, columns):
    size = width * LANES
    full = []
    for j, column in enumerate(columns):
        spare = size - column.shape[0]
        full.append(jnp.concatenate([column, jnp.zeros((spare, LANES), jnp.float32)], axis=0) if spare else column)
    return jnp.concatenate(full, axis=1)


def from_rows(width, rows):
    size = width * LANES
    full = []
    for row in rows:
        spare = size - row.shape[1]
        full.append(jnp.concatenate([jnp.zeros((LANES, spare), jnp.float32), row], axis=1) if spare else row)
    return jnp.concatenate(full, axis=0)


def symmetric_half(width, grad, upper):
    row, lane = iotas(grad.shape)
    kept = jnp.where(row <= lane, grad, 0.0)
    columns = []
    for j in range(width):
        at = j * LANES
        columns.append(dot3(kept[0 : at + LANES, at:], upper[at : at + LANES, at:], NT))
    product = from_columns(width, columns)
    phi = jnp.where(row < lane, product, jnp.where(row == lane, 0.5 * product, 0.0))
    return 0.5 * (phi + phi.T), phi


def whole_kernel(counts, width, matrix_in, q_grad_in, grad_factor_in, out, *scratch):
    scratch = list(scratch)

    def take(count):
        taken = scratch[:count]
        del scratch[:count]
        return taken

    row, core = lax.axis_index("rows"), lax.axis_index("sub")
    size = width * LANES
    rate = shift_frac / size
    last = width - 1
    pairs = [(i, b) for b in range(width) for i in range(b + 1)]
    all_sums = summers(counts, width)
    head, rest, later, off, cross = all_sums
    for summer in flat(all_sums):
        summer.bind(row, core, *take(len(summer.scratch())))
    matrix, q_grad, grad_factor, loads, work, upper1, inverse1, upper2, inverse2, current, held, early, gram2, moved, after, turning = scratch

    loading = []
    for index, (source, target) in enumerate(
        [(matrix_in, matrix), (q_grad_in, q_grad), (grad_factor_in, grad_factor)]
    ):
        loading.append(pltpu.make_async_copy(source, target, loads.at[index]))
        loading[-1].start()
    greet(counts, row, core)
    loading[0].wait()
    squares = jnp.sum(matrix[...] * matrix[...])
    line, lane = iotas((LANES, LANES))
    corner = (line == LANES - 1) & (lane == 0)
    head.put(jnp.where(corner, squares, dot6(matrix[:, block(0)], matrix[:, block(0)], TN)))
    greeted(counts)
    head.start()
    for b in range(1, width):
        for i in range(b + 1):
            rest[b - 1].put(i, dot6(matrix[:, block(i)], matrix[:, block(b)], TN))
        rest[b - 1].pair_start()
    loading[1].wait()
    for index, (i, j) in enumerate(pairs):
        cross.put(index, dot6(matrix[:, block(i)], q_grad[:, block(j)], TN))
    cross.pair_start()
    loading[2].wait()
    for summer in rest:
        summer.pair_add()
        summer.scatter()
    cross.pair_add()
    head.reduce()
    for summer in rest:
        summer.reduce()
    head.gathered()
    first_block = head.get(0, LANES)
    shift1 = rate * jnp.broadcast_to(first_block[LANES - 1 : LANES, 0:1], (1, LANES))
    first_block = jnp.where(corner, first_block[0:1, LANES - 1 : LANES], first_block)

    def rest_share():
        for summer in rest[1:]:
            summer.share()

    def between_on():
        for summer in later[1:-1]:
            summer.pair_add()
            summer.scatter()
        later[0].reduce()

    def off_start(carried):
        ahead = matrix[:, block(last)] - dot6(matrix[:, upto(last)], carried, NT)
        for i in range(last):
            off.put(i, dot6(current[:, block(i)], ahead, TN))
        off.pair_start()

    def off_on():
        off.pair_add()
        off.scatter()

    def gram1(b):
        above = jnp.concatenate([rest[b - 1].get(i) for i in range(b)], axis=0)
        return rest[b - 1].get(b), prepare(b, above, upper1, inverse1)

    hooks1 = {
        0: {2: rest[0].share},
        1: {1: rest_share},
        last: {0: between_on, 3: off_on},
    }
    diagonal, prepared = first_block, None
    for b in range(width):
        hooks = hooks1.get(b, {})
        if b == last:
            hooks = {**hooks, 1: functools.partial(off_start, prepared[1])}
        factor_column(b, diagonal, prepared, shift1, work, upper1, inverse1, hooks)
        if b < last:
            rest[b].shared()
        current[:, block(b)] = dot6(matrix[:, upto(b + 1)], inverse1[block(b), upto(b + 1)], NT)
        if b in (0, last):
            later[b].put(dot6(current[:, block(b)], current[:, block(b)], TN))
        else:
            for i in range(b + 1):
                later[b].put(i, dot6(current[:, block(i)], current[:, block(b)], TN))
        if b < last:
            diagonal, prepared = gram1(b + 1)
        if b in (0, last):
            later[b].start()
        else:
            later[b].pair_start()
        if b == 0:
            cross.scatter()
    for summer in later[1:-1]:
        summer.reduce()
    inverse = inverse1[...]
    shift2 = rate * (size - shift1 * jnp.sum(inverse * inverse))

    def early_on():
        columns = []
        for j in range(width):
            at = j * LANES
            columns.append(dot3(grad_factor[0 : at + LANES, at:], upper1[at : at + LANES, at:], NT))
        early[...] = from_columns(width, columns)

    def off_above():
        off.shared()
        above = jnp.concatenate([off.get(i) for i in range(last)], axis=0)
        gram2[upto(last), block(last)] = dot6(above, inverse1[block(last), block(last)], NT)

    def cross_on():
        cross.shared()
        crossed = [
            jnp.concatenate([cross.get(pairs.index((i, j))) for j in range(i, width)], axis=1) for i in range(width)
        ]
        held[...] = from_rows(width, lower_times_upper(width, inverse1, from_rows(width, crossed), dot6))

    def known_parts():
        for i in range(last):
            at = i * LANES
            moved[at : at + LANES, at:] = dot3(
                upper2[0 : at + LANES, at : at + LANES], grad_factor[0 : at + LANES, at:], TN
            )
        after[:, upto(last)] = dot3(current[:, upto(last)], inverse2[upto(last), upto(last)], NT)
        turning[:, upto(last)] = dot3(q_grad[:, upto(last)], inverse2[upto(last), upto(last)])

    def later_on():
        later[-1].reduce()
        for summer in later[1:-1]:
            summer.share()
        cross.reduce()

    hooks2 = {
        0: {1: early_on, 2: off.reduce, 3: later_on},
        1: {2: off.share, 3: off_above},
        last: {1: known_parts, 2: cross.share, 3: cross_on},
    }
    for b in range(width):
        if b == last:
            prepared = prepare(b, gram2[upto(b), block(b)], upper2, inverse2)
            later[b].gathered()
            diagonal = later[b].get(0, LANES)
            gram2[block(b), block(b)] = diagonal
        else:
            if b:
                later[b].shared()
                column = jnp.concatenate([later[b].get(i) for i in range(b + 1)], axis=0)
            else:
                later[b].gathered()
                column = later[b].get(0, LANES)
            gram2[upto(b + 1), block(b)] = column
            diagonal = column[b * LANES :, :]
            prepared = prepare(b, column[: b * LANES, :], upper2, inverse2) if b else None
        factor_column(b, diagonal, prepared, shift2, work, upper2, inverse2, hooks2.get(b, {}))
    row, lane = iotas((size, size))
    inverse = inverse2[...]
    turned = from_columns(width, upper_times_lower(width, held[...], inverse))
    total2 = early[...] - from_rows(width, lower_times_upper(width, inverse, turned))
    half2, _ = symmetric_half(width, total2, upper2)
    middle = jnp.concatenate(
        [dot3(half2[:, j * LANES :], inverse[j * LANES :, j * LANES : (j + 1) * LANES]) for j in range(width)], axis=1
    )
    trace2 = rate * jnp.sum(middle * inverse)
    gram = jnp.where(row // LANES <= lane // LANES, gram2[...], 0.0)
    wide2 = jnp.concatenate([shift2] * width, axis=1)
    mixed = upper2[...] - wide2 * inverse
    across = from_columns(
        width,
        [
            dot3(mixed[:, 0 : (j + 1) * LANES], middle[:, j * LANES : (j + 1) * LANES], TN)
            for j in range(width)
        ],
    )
    crossed1 = turned + 2.0 * (across + trace2 * gram)
    moved[block(last), block(last)] = dot3(upper2[:, block(last)], grad_factor[:, block(last)], TN)
    kept = jnp.where(row // LANES <= lane // LANES, moved[...], 0.0)
    total1 = kept - from_columns(width, upper_times_lower(width, crossed1, inverse1))
    half1, phi1 = symmetric_half(width, total1, upper1)
    missing = jnp.where(row == lane, 1.0 - gram, -gram)
    trace1 = rate * jnp.sum(phi1 * missing) / shift1
    after[:, block(last)] = dot3(current[...], inverse[last * LANES :, :], NT)
    turned_grad = dot3(q_grad[:, block(last)], inverse[last * LANES :, :])
    turned_grad = turned_grad + jnp.concatenate(
        [turning[:, upto(last)], jnp.zeros((q_grad.shape[0], LANES), jnp.float32)], axis=1
    )
    grad = turned_grad + 2.0 * (dot3(after[...], middle) + trace2 * current[...])
    grad = grad + 2.0 * dot3(current[...], half1)
    wide1 = jnp.concatenate([trace1] * width, axis=1)
    out[...] = dot3(grad, inverse1[...]) + 2.0 * wide1 * matrix[...]
    for summer in flat(all_sums):
        summer.settle()


def summers(counts, width):
    count = width * (width + 1) // 2
    rest = [Paired(counts, (b + 1) * LANES) for b in range(1, width)]
    later = [Direct(counts, LANES)] + [Paired(counts, (b + 1) * LANES) for b in range(1, width - 1)] + [Direct(counts, LANES)]
    off = Paired(counts, (width - 1) * LANES)
    return Direct(counts, LANES), rest, later, off, Paired(counts, count * LANES)


def flat(sums):
    head, rest, later, off, cross = sums
    return [head, *rest, *later, off, cross]


def per_device(counts, matrix, grad_out, grad_factor):
    rows, size = matrix.shape
    width = size // LANES
    vmem = pl.BlockSpec(memory_space=pltpu.VMEM)
    square = pltpu.VMEM((size, size), jnp.float32)
    tall = pltpu.VMEM((rows, size), jnp.float32)
    work = pltpu.VMEM((LANES, 2 * LANES), jnp.float32)
    sums = []
    for summer in flat(summers(counts, width)):
        sums = sums + summer.scratch()
    held = [tall, tall, square, pltpu.SemaphoreType.DMA((3,)), work] + [square] * 4 + [tall, square, square] + [square, square, tall, tall]
    return pl.pallas_call(
        functools.partial(whole_kernel, counts, width),
        out_shape=pltpu.VMEM((rows, size), jnp.float32),
        in_specs=[pl.BlockSpec(memory_space=pl.ANY)] * 3,
        out_specs=vmem,
        scratch_shapes=sums + held,
        compiler_params=pltpu.CompilerParams(
            vmem_limit_bytes=VMEM_LIMIT, collective_id=0, has_side_effects=True
        ),
    )(matrix, grad_out, grad_factor)


def solution(mesh):
    counts = (mesh.shape["rows"], mesh.shape["sub"])
    placed = (P(("rows", "sub"), None), P(("rows", "sub"), None), P())
    return jax.shard_map(
        functools.partial(per_device, counts),
        mesh=mesh,
        in_specs=placed,
        out_specs=P(("rows", "sub"), None),
        check_vma=False,
    )
```
